128 devices in a mesh: region: 16 (over y_lo, z, core), depth: 2 (over y_hi), member: 4 (over x).
Axes of the slice: x: 4, y: 4 (y_hi: 2, y_lo: 2; y = y_hi * 2 + y_lo), z: 4, core: 2. Of those that a mesh axis runs over, the one named last changes fastest.
Arguments:
- ensemble: bfloat16 [14, 384, 16384], P('depth', 'member', 'region'), may hold values from -6 to 6
- obs_weights: float32 [14], P('depth'), may hold values from -1.5 to 1.5
- obs_tiles: int32 [8192], P('region'), may hold values from 0 to 1023
- obs_values: float32 [8192], P('region'), may hold values from -8 to 8
- obs_error: float32 [8192], P('region'), may hold values from 0.2 to 2
- obs_noise: float32 [384, 8192], P('member', 'region'), may hold values from -6 to 6
Outputs:
- analysis: bfloat16 [14, 384, 16384], P('depth', 'member', 'region')
- inflation: float32 [], replicated
The draws below stay inside these ranges and needn't reach their ends.
Inputs may be any that keep to these rules, and one draw needn't show every extreme that they name: `obs_tiles`: the tile of the observation, counted within the 1024 tiles of the region whose block holds the observation.
All inputs are finite; a program needn't handle non-finite values.
Results may differ from the reference program's by a relative error of at most 0.011.
Values may be sent and summed in bfloat16 or wider, within the bound.
No kernel may reach another device: no remote copies, remote signals or barrier semaphores. Data moves between devices by JAX's collectives and lax.ppermute only.
A program may use at most 64 MiB of HBM per device.

```python
import math
import jax
import jax.numpy as jnp
from jax import lax

VARS = 14
MEMBERS = 384
TILE_DEV = 1024
OBS_DEV = 512
NTILES = 16384
NOBS = 8192
RADIUS = 1024
N_REGION = 16


def touch_ends(values, own_key, smallest, largest):
    shape = values.shape
    spot = [jax.random.randint(jax.random.fold_in(own_key, axis), (), 0, shape[axis]) for axis in range(len(shape))]
    values = values.at[tuple(spot)].set(smallest)
    longest = shape.index(max(shape))
    spot[longest] = (spot[longest] + 1) % shape[longest]
    return values.at[tuple(spot)].set(largest)


def block_levels(key, dims, cuts, least, top_value):
    level = 1.0
    for dim, blocks in cuts:
        draws = jax.random.uniform(jax.random.fold_in(jax.random.fold_in(key, 6), dim), (blocks,), jnp.float32, least / len(cuts), top_value / len(cuts))
        level = level * jnp.repeat(jnp.exp(draws), dims[dim] // blocks).reshape((-1,) + (1,) * (len(dims) - 1 - dim))
    return level


def gaussian(key, dims, scale, limit, split=(), kind=jnp.bfloat16):
    factor_of = block_levels(key, dims, split, -0.22, 0.18) if split else 1.0
    drawn = jax.random.normal(key, dims, jnp.float32) * scale * factor_of
    return jnp.minimum(jnp.maximum(drawn, -limit), limit).astype(kind)


def setup_inputs(seed: int = 0) -> dict:
    splits = jax.random.split(jax.random.key(seed), 7)
    return {
        "ensemble": gaussian(splits[0], (VARS, MEMBERS, NTILES), 1.0, 6.0, ((0, 2), (1, 4), (2, 16))),
        "obs_weights": gaussian(splits[1], (VARS,), VARS ** -0.5, 1.5, ((0, 2),), jnp.float32),
        "obs_tiles": touch_ends(jax.random.randint(splits[2], (NOBS,), 0, TILE_DEV), jax.random.fold_in(splits[2], 1), 0, TILE_DEV - 1).astype(jnp.int32),
        "obs_values": gaussian(splits[3], (NOBS,), 2.0, 8.0, ((0, 16),), jnp.float32),
        "obs_error": jnp.clip(jnp.exp(math.log(2.0) - 2.3025851 * jax.random.uniform(splits[4], (NOBS,), jnp.float32) ** block_levels(splits[4], (NOBS,), ((0, 16),), -0.2, 0.2)), 0.2, 2.0),
        "obs_noise": gaussian(splits[5], (MEMBERS, NOBS), 1.0, 6.0, ((0, 4), (1, 16)), jnp.float32),
    }


def reference(ensemble, obs_weights, obs_tiles, obs_values, obs_error, obs_noise):
    state_f = ensemble.astype(jnp.float32)
    state_mean = lax.optimization_barrier(jnp.sum(state_f, axis=1)) / MEMBERS
    anomalies = (state_f - state_mean[:, None, :]).astype(jnp.bfloat16)
    obs_region = jnp.arange(NOBS, dtype=jnp.int32) // OBS_DEV
    obs_global = obs_region * TILE_DEV + obs_tiles.astype(jnp.int32)
    picked = jnp.take(ensemble, obs_global, axis=2).astype(jnp.float32)
    predicted = jnp.einsum('lmk,l->mk', picked, obs_weights.astype(jnp.float32), precision=lax.Precision.HIGHEST)
    obs_mean = lax.optimization_barrier(jnp.sum(predicted, axis=0)) / MEMBERS
    obs_dev = predicted - obs_mean[None, :]
    obs_spread = lax.optimization_barrier(jnp.sum(obs_dev * obs_dev, axis=0)) / (MEMBERS - 1)
    innovation = obs_values - obs_mean
    inflation = jnp.sum(innovation * innovation) / jnp.sum(obs_spread + obs_error)
    infl_root = jnp.sqrt(inflation)
    factor = inflation / (inflation * obs_spread + obs_error)
    obs_anom = obs_dev.astype(jnp.bfloat16)
    perturbed = (innovation[None, :] + jnp.sqrt(obs_error)[None, :] * obs_noise - infl_root * obs_dev).astype(jnp.bfloat16)
    padded_anom = jnp.pad(obs_anom, ((0, 0), (OBS_DEV, OBS_DEV)))
    padded_pert = jnp.pad(perturbed, ((0, 0), (OBS_DEV, OBS_DEV)))
    padded_factor = jnp.pad(factor, (OBS_DEV, OBS_DEV))
    padded_pos = jnp.pad(obs_global.astype(jnp.float32), (OBS_DEV, OBS_DEV))

    def one_region(region_id):
        first_obs = region_id * OBS_DEV
        anom_window = lax.dynamic_slice_in_dim(padded_anom, first_obs, 3 * OBS_DEV, 1).astype(jnp.float32)
        pert_window = lax.dynamic_slice_in_dim(padded_pert, first_obs, 3 * OBS_DEV, 1).astype(jnp.float32)
        factor_window = lax.dynamic_slice_in_dim(padded_factor, first_obs, 3 * OBS_DEV, 0)
        pos_window = lax.dynamic_slice_in_dim(padded_pos, first_obs, 3 * OBS_DEV, 0)
        first_tile = region_id * TILE_DEV
        region_anom = lax.dynamic_slice_in_dim(anomalies, first_tile, TILE_DEV, 2).astype(jnp.float32)
        region_mean = lax.dynamic_slice_in_dim(state_mean, first_tile, TILE_DEV, 1)
        covariance = jnp.einsum('lmt,mj->ltj', region_anom, anom_window) / (MEMBERS - 1)
        tile_pos = (first_tile + jnp.arange(TILE_DEV, dtype=jnp.int32)).astype(jnp.float32)
        closeness = jnp.maximum(0.0, 1.0 - jnp.abs(tile_pos[:, None] - pos_window[None, :]) / RADIUS)
        kalman_gain = (covariance * (closeness * closeness * factor_window[None, :])[None]).astype(jnp.bfloat16)
        increment = jnp.einsum('ltj,mj->lmt', kalman_gain.astype(jnp.float32), pert_window)
        return (region_mean[:, None, :] + infl_root * region_anom + increment).astype(jnp.bfloat16)
    region_out = lax.map(one_region, jnp.arange(N_REGION, dtype=jnp.int32))
    analysis = jnp.transpose(region_out, (1, 2, 0, 3)).reshape(VARS, MEMBERS, NTILES)
    return (analysis, inflation)
```

```python
import functools

import jax
import jax.numpy as jnp
from jax import lax
from jax.experimental import pallas as pl
from jax.experimental.pallas import tpu as pltpu
from jax.sharding import PartitionSpec as P

RADIUS = 1024
F32 = jnp.float32
BF16 = jnp.bfloat16


def params(**more):
    return pltpu.CompilerParams(vmem_limit_bytes=56 * 2**20, **more)


def whole():
    return pl.BlockSpec(memory_space=pltpu.VMEM)


def scalars():
    return pl.BlockSpec(memory_space=pltpu.SMEM)


def shape_of(shape, dtype=BF16):
    return jax.ShapeDtypeStruct(shape, dtype)


def split_rows(value):
    first = value.astype(BF16)
    rest = value - first.astype(F32)
    second = rest.astype(BF16)
    third = (rest - second.astype(F32)).astype(BF16)
    return [first, second, third]


def pack_body(weights, ensemble, tiles, blocks, predicted, total):
    step = pl.program_id(0)
    var_count, _, width = ensemble.shape
    blocks[0] = ensemble[...]
    mixed = weights[0] * ensemble[0].astype(F32)
    for l in range(1, var_count):
        mixed = mixed + weights[l] * ensemble[l].astype(F32)
    high = mixed.astype(BF16)
    low = (mixed - high.astype(F32)).astype(BF16)
    rows = lax.broadcasted_iota(jnp.int32, (width, tiles.shape[1]), 0)
    chosen = jnp.where(tiles[...] - step * width == rows, 1.0, 0.0).astype(BF16)
    picked = jnp.dot(high, chosen, preferred_element_type=F32)
    picked = picked + jnp.dot(low, chosen, preferred_element_type=F32)

    @pl.when(step == 0)
    def _():
        total[...] = picked

    @pl.when(step > 0)
    def _():
        total[...] += picked

    @pl.when(step == pl.num_programs(0) - 1)
    def _():
        predicted[...] = total[...].astype(BF16)


def pack(ensemble, weights, tiles, peers):
    var_count, own, tile_count = ensemble.shape
    width = tile_count // peers
    obs = tiles.shape[1]
    return pl.pallas_call(
        pack_body,
        grid=(peers,),
        in_specs=[
            scalars(),
            pl.BlockSpec((var_count, own, width), lambda j: (0, 0, j)),
            pl.BlockSpec((1, obs), lambda j: (0, 0)),
        ],
        out_specs=[
            pl.BlockSpec((1, var_count, own, width), lambda j: (j, 0, 0, 0)),
            pl.BlockSpec((own, obs), lambda j: (0, 0)),
        ],
        out_shape=[shape_of((peers, var_count, own, width)), shape_of((own, obs))],
        scratch_shapes=[pltpu.VMEM((own, obs), F32)],
        compiler_params=params(),
        name="pack",
    )(weights, ensemble, tiles)


def join_body(mine, other, noise, error, out):
    own = mine.shape[0]
    predicted = (mine[...].astype(F32) + other[...].astype(F32)).astype(BF16)
    scaled = (jnp.sqrt(error[...]) * noise[...]).astype(BF16)
    for j in range(out.shape[0]):
        out[j, :own] = predicted
        out[j, own:] = scaled


def join(mine, other, noise, error, peers):
    own, obs = mine.shape
    return pl.pallas_call(
        join_body,
        in_specs=[whole()] * 4,
        out_specs=whole(),
        out_shape=shape_of((peers, 2 * own, obs)),
        compiler_params=params(),
        name="join",
    )(mine, other, noise, error)


def stats_body(gathered, values, error, tiles, packet, sums):
    peers, double, obs = gathered.shape
    own = double // 2
    members = peers * own
    total = jnp.zeros((1, obs), F32)
    for j in range(peers):
        total = total + jnp.sum(gathered[j, :own].astype(F32), axis=0, keepdims=True)
    mean = total / members
    square = jnp.zeros((1, obs), F32)
    for j in range(peers):
        dev = gathered[j, :own].astype(F32) - mean
        square = square + jnp.sum(dev * dev, axis=0, keepdims=True)
        packet[j * own : (j + 1) * own] = dev.astype(BF16)
        packet[members + j * own : members + (j + 1) * own] = gathered[j, own:]
    spread = square / (members - 1)
    innovation = values[...] - mean
    place = tiles[...]
    rows = split_rows(innovation) + split_rows(error[...]) + split_rows(spread)
    rows += [(place // 32).astype(F32).astype(BF16), (place % 32).astype(F32).astype(BF16)]
    rows += [jnp.zeros((1, obs), BF16)] * (16 - len(rows))
    packet[2 * members :] = jnp.concatenate(rows, axis=0)
    above = jnp.sum(innovation * innovation)
    below = jnp.sum(spread + error[...])
    lane = lax.broadcasted_iota(jnp.int32, sums.shape, 1)
    sums[...] = jnp.where(lane == 0, above, jnp.where(lane == 1, below, 0.0))


def stats(gathered, values, error, tiles, regions):
    peers, double, obs = gathered.shape
    return pl.pallas_call(
        stats_body,
        in_specs=[whole()] * 4,
        out_specs=[whole(), whole()],
        out_shape=[shape_of((peers * double + 16, obs)), shape_of((regions, 128), F32)],
        compiler_params=params(),
        name="stats",
    )(gathered, values, error, tiles)


def prepare_body(offset, left, mine, right, sums, anom_t, perturbed, taper, inflation_out, *, tile_count):
    total, obs = mine.shape
    members = (total - 16) // 2
    width = taper.shape[1]
    folded = jnp.sum(sums[...], axis=0, keepdims=True)
    inflation = folded[:, 0:1] / folded[:, 1:2]
    root = jnp.sqrt(inflation)
    inflation_out[...] = jnp.broadcast_to(inflation, inflation_out.shape)
    tile = (offset[0] + lax.broadcasted_iota(jnp.int32, (1, width), 1)).astype(F32)
    for n, packet in enumerate((left, mine, right)):
        anom = packet[:members]
        anom_t[n * obs : (n + 1) * obs] = anom.T
        rows = packet[2 * members :].astype(F32)
        innovation = rows[0:1] + rows[1:2] + rows[2:3]
        error = rows[3:4] + rows[4:5] + rows[5:6]
        spread = rows[6:7] + rows[7:8] + rows[8:9]
        place = rows[9:10] * 32.0 + rows[10:11] + (n - 1.0) * tile_count
        scaled = packet[members : 2 * members].astype(F32)
        perturbed[:, n * obs : (n + 1) * obs] = (
            innovation + scaled - root * anom.astype(F32)
        ).astype(BF16)
        bottom = inflation * spread + error
        factor = jnp.where(error > 0.0, inflation / jnp.where(error > 0.0, bottom, 1.0), 0.0)
        factor = factor / (members - 1)
        columns = jnp.concatenate([place, factor, jnp.zeros((6, obs), F32)], axis=0).T
        near = jnp.maximum(0.0, 1.0 - jnp.abs(tile - columns[:, 0:1]) / RADIUS)
        taper[n * obs : (n + 1) * obs] = near * near * columns[:, 1:2]


def prepare(offset, left, mine, right, sums, width, tile_count):
    total, obs = mine.shape
    members = (total - 16) // 2
    return pl.pallas_call(
        functools.partial(prepare_body, tile_count=tile_count),
        in_specs=[scalars()] + [whole()] * 4,
        out_specs=[whole()] * 4,
        out_shape=[
            shape_of((3 * obs, members)),
            shape_of((members, 3 * obs)),
            shape_of((3 * obs, width), F32),
            shape_of((8, 128), F32),
        ],
        compiler_params=params(),
        name="prepare",
    )(offset, left, mine, right, sums)


def regress_body(states, anom_t, perturbed, taper, inflation, out, gain, *, first, count):
    peers, _, own, width = states.shape
    members = peers * own
    root = jnp.sqrt(inflation[0:1, 0:1])
    obs = taper.shape[0]
    block = 512

    def one(l, carry):
        state = states[:, first + l].astype(F32).reshape(members, width)
        mean = jnp.sum(state, axis=0, keepdims=True) / members
        anom = (state - mean).astype(BF16)
        for k in range(0, obs, block):
            covariance = jnp.dot(anom_t[k : k + block], anom, preferred_element_type=F32)
            gain[k : k + block] = (covariance * taper[k : k + block]).astype(BF16)
        increment = jnp.dot(perturbed[...], gain[...], preferred_element_type=F32)
        result = mean + root * anom.astype(F32) + increment
        out[:, l] = result.astype(BF16).reshape(peers, own, width)
        return carry

    lax.fori_loop(0, count, one, 0)


def regress(states, anom_t, perturbed, taper, inflation, first, count):
    peers, _, own, width = states.shape
    return pl.pallas_call(
        functools.partial(regress_body, first=first, count=count),
        in_specs=[whole()] * 5,
        out_specs=whole(),
        out_shape=shape_of((peers, count, own, width)),
        scratch_shapes=[pltpu.VMEM(taper.shape, BF16)],
        compiler_params=params(),
        name=f"regress{first}",
    )(states, anom_t, perturbed, taper, inflation)


def place_body(first, second, out):
    count = first.shape[1]
    out[:count] = first[0]
    out[count:] = second[0]


def place(first, second):
    peers, count, own, width = first.shape
    rest = second.shape[1]
    return pl.pallas_call(
        place_body,
        grid=(peers,),
        in_specs=[
            pl.BlockSpec((1, count, own, width), lambda j: (j, 0, 0, 0)),
            pl.BlockSpec((1, rest, own, width), lambda j: (j, 0, 0, 0)),
        ],
        out_specs=pl.BlockSpec((count + rest, own, width), lambda j: (0, 0, j)),
        out_shape=shape_of((count + rest, own, peers * width)),
        compiler_params=params(),
        name="place",
    )(first, second)


def exchanged(blocks, axis):
    return lax.all_to_all(blocks, axis, split_axis=0, concat_axis=0, tiled=True)


def shards(ensemble, obs_weights, obs_tiles, obs_values, obs_error, obs_noise):
    peers = lax.axis_size("member")
    regions = lax.axis_size("region")
    width = ensemble.shape[2] // peers
    tiles, values, error = (a[None, :] for a in (obs_tiles, obs_values, obs_error))
    blocks, partial = pack(ensemble, obs_weights, tiles, peers)
    other = lax.ppermute(partial, "depth", [(0, 1), (1, 0)])
    states = exchanged(blocks, "member")
    gathered = exchanged(join(partial, other, obs_noise, error, peers), "member")
    packet, sums = stats(gathered, values, error, tiles, regions)
    up = [(i, i + 1) for i in range(regions - 1)]
    left = lax.ppermute(packet, "region", up)
    right = lax.ppermute(packet, "region", [(j, i) for i, j in up])
    all_sums = exchanged(sums, "region")
    offset = (lax.axis_index("member") * width).astype(jnp.int32)[None]
    anom_t, perturbed, taper, inflation = prepare(
        offset, left, packet, right, all_sums, width, ensemble.shape[2]
    )
    count = ensemble.shape[0]
    half = (count + 1) // 2
    parts = []
    for first, size in ((0, half), (half, count - half)):
        updated = regress(states, anom_t, perturbed, taper, inflation, first, size)
        parts.append(exchanged(updated, "member"))
    return (place(*parts), inflation[0, 0])


def solution(mesh):
    return jax.shard_map(
        shards,
        mesh=mesh,
        in_specs=(
            P("depth", "member", "region"),
            P("depth"),
            P("region"),
            P("region"),
            P("region"),
            P("member", "region"),
        ),
        out_specs=(P("depth", "member", "region"), P()),
        check_vma=False,
    )
```

```python
import functools

import jax
import jax.numpy as jnp
from jax import lax
from jax.experimental import pallas as pl
from jax.experimental.pallas import tpu as pltpu
from jax.sharding import PartitionSpec as P


RADIUS = 1024
F32 = jnp.float32
BF16 = jnp.bfloat16


def params(megabytes=12):
    return pltpu.CompilerParams(vmem_limit_bytes=megabytes * 2**20)


def whole():
    return pl.BlockSpec(memory_space=pltpu.VMEM)


def scalars():
    return pl.BlockSpec(memory_space=pltpu.SMEM)


def anywhere():
    return pl.BlockSpec(memory_space=pl.ANY)


def shape_of(shape, dtype=BF16):
    return pltpu.VMEM(shape, dtype)


def in_vmem(values):
    return [pltpu.with_memory_space_constraint(v, pltpu.VMEM) for v in values]


def split_rows(value):
    first = value.astype(BF16)
    rest = value - first.astype(F32)
    second = rest.astype(BF16)
    third = (rest - second.astype(F32)).astype(BF16)
    return [first, second, third]


def tile_block(me, s, width):
    return pl.multiple_of(jnp.bitwise_xor(me, s) * width, width)


def pack_body(me, weights, ensemble, tiles, *rest):
    *blocks, predicted, arrived = rest
    peers = len(blocks)
    var_count, _, width = blocks[0].shape
    starts = [tile_block(me[0], s, width) for s in range(peers)]
    loads = [
        pltpu.make_async_copy(
            ensemble.at[:, :, pl.ds(starts[s], width)], blocks[s], arrived.at[s]
        )
        for s in range(peers)
    ]
    for load in loads:
        load.start()
    rows = lax.broadcasted_iota(jnp.int32, (width, tiles.shape[1]), 0)
    total = jnp.zeros(predicted.shape, F32)
    for s in range(peers):
        chosen = jnp.where(tiles[...] - starts[s] == rows, 1.0, 0.0).astype(BF16)
        loads[s].wait()
        mixed = weights[0] * blocks[s][0].astype(F32)
        for l in range(1, var_count):
            mixed = mixed + weights[l] * blocks[s][l].astype(F32)
        high = mixed.astype(BF16)
        low = (mixed - high.astype(F32)).astype(BF16)
        total = total + jnp.dot(high, chosen, preferred_element_type=F32)
        total = total + jnp.dot(low, chosen, preferred_element_type=F32)
    predicted[...] = total.astype(BF16)


def pack(me, ensemble, weights, tiles, peers):
    var_count, own, tile_count = ensemble.shape
    width = tile_count // peers
    obs = tiles.shape[1]
    return pl.pallas_call(
        pack_body,
        in_specs=[scalars(), scalars(), anywhere(), whole()],
        out_specs=[whole()] * (peers + 1),
        out_shape=[shape_of((var_count, own, width))] * peers + [shape_of((own, obs))],
        scratch_shapes=[pltpu.SemaphoreType.DMA((peers,))],
        compiler_params=params(),
        name="pack",
    )(me, weights, pltpu.with_memory_space_constraint(ensemble, pltpu.HBM), tiles)


def join_body(mine, other, noise, error, out):
    own = mine.shape[0]
    predicted = (mine[...].astype(F32) + other[...].astype(F32)).astype(BF16)
    scaled = (jnp.sqrt(error[...]) * noise[...]).astype(BF16)
    for j in range(out.shape[0]):
        out[j, :own] = predicted
        out[j, own:] = scaled


def join(mine, other, noise, error, peers):
    own, obs = mine.shape
    return pl.pallas_call(
        join_body,
        in_specs=[whole()] * 4,
        out_specs=whole(),
        out_shape=shape_of((peers, 2 * own, obs)),
        compiler_params=params(),
        name="join",
    )(mine, other, noise, error)


def stats_body(me, gathered, values, error, tiles, packet, sums):
    peers, double, obs = gathered.shape
    own = double // 2
    members = peers * own
    total = jnp.zeros((1, obs), F32)
    for j in range(peers):
        total = total + jnp.sum(gathered[j, :own].astype(F32), axis=0, keepdims=True)
    mean = total / members
    square = jnp.zeros((1, obs), F32)
    for j in range(peers):
        dev = gathered[j, :own].astype(F32) - mean
        square = square + jnp.sum(dev * dev, axis=0, keepdims=True)
    for s in range(peers):
        j = jnp.bitwise_xor(me[0], s)
        dev = gathered[j, :own].astype(F32) - mean
        packet[s * own : (s + 1) * own] = dev.astype(BF16)
        packet[members + s * own : members + (s + 1) * own] = gathered[j, own:]
    spread = square / (members - 1)
    innovation = values[...] - mean
    place = tiles[...]
    rows = split_rows(innovation) + split_rows(error[...]) + split_rows(spread)
    rows += [(place // 32).astype(F32).astype(BF16), (place % 32).astype(F32).astype(BF16)]
    rows += [jnp.zeros((1, obs), BF16)] * (16 - len(rows))
    packet[2 * members :] = jnp.concatenate(rows, axis=0)
    above = jnp.sum(innovation * innovation)
    below = jnp.sum(spread + error[...])
    lane = lax.broadcasted_iota(jnp.int32, sums.shape, 1)
    sums[...] = jnp.where(lane == 0, above, jnp.where(lane == 1, below, 0.0))


def stats(me, gathered, values, error, tiles, regions):
    peers, double, obs = gathered.shape
    return pl.pallas_call(
        stats_body,
        in_specs=[scalars()] + [whole()] * 4,
        out_specs=[whole(), whole()],
        out_shape=[shape_of((peers * double + 16, obs)), shape_of((regions, 128), F32)],
        compiler_params=params(),
        name="stats",
    )(me, gathered, values, error, tiles)


def scalar_rows(packet, members):
    rows = packet[2 * members :].astype(F32)
    innovation = rows[0:1] + rows[1:2] + rows[2:3]
    error = rows[3:4] + rows[4:5] + rows[5:6]
    spread = rows[6:7] + rows[7:8] + rows[8:9]
    return innovation, error, spread, rows[9:10] * 32.0 + rows[10:11]


def gains_body(offset, *refs, tile_count, peers):
    states, packets = refs[:peers], refs[peers : peers + 3]
    gain, anomalies, means, anom_t, taper = refs[peers + 3 :]
    var_count, own, width = states[0].shape
    members = peers * own
    obs = packets[0].shape[1]
    tile = (offset[0] + lax.broadcasted_iota(jnp.int32, (1, width), 1)).astype(F32)
    for n, packet in enumerate(packets):
        anom_t[n * obs : (n + 1) * obs] = packet[:members].T
        place = scalar_rows(packet, members)[3] + (offset[1 + n] * tile_count).astype(F32)
        column = jnp.broadcast_to(place, (8, obs)).T[:, 0:1]
        near = jnp.maximum(0.0, 1.0 - jnp.abs(tile - column) / RADIUS)
        taper[n * obs : (n + 1) * obs] = near * near / (members - 1)
    for l in range(var_count):
        state = [states[s][l].astype(F32) for s in range(peers)]
        total = sum(jnp.sum(a, axis=0, keepdims=True) for a in state)
        mean = total / members
        means[l] = jnp.broadcast_to(mean, means.shape[1:])
        for s in range(peers):
            anomalies[l, s * own : (s + 1) * own] = (state[s] - mean).astype(BF16)
        for k in range(0, 3 * obs, obs):
            covariance = jnp.dot(anom_t[k : k + obs], anomalies[l], preferred_element_type=F32)
            gain[l, k : k + obs] = (covariance * taper[k : k + obs]).astype(BF16)


def gains(offset, states, packets, tile_count):
    var_count, own, width = states[0].shape
    peers = len(states)
    members = peers * own
    obs = packets[0].shape[1]
    return pl.pallas_call(
        functools.partial(gains_body, tile_count=tile_count, peers=peers),
        in_specs=[scalars()] + [whole()] * (peers + 3),
        out_specs=[whole()] * 3,
        out_shape=[
            shape_of((var_count, 3 * obs, width)),
            shape_of((var_count, members, width)),
            shape_of((var_count, 8, width), F32),
        ],
        scratch_shapes=[pltpu.VMEM((3 * obs, members), BF16), pltpu.VMEM((3 * obs, width), F32)],
        compiler_params=params(),
        name="gains",
    )(offset, *in_vmem(states), *in_vmem(packets))


def update(gain, anomalies, means, perturbed, root, blocks, l, at):
    own = blocks[0].shape[1]
    increment = jnp.dot(perturbed[...], gain[l], preferred_element_type=F32)
    result = means[l, 0:1] + root * anomalies[l].astype(F32) + increment
    for s, block in enumerate(blocks):
        block[at] = result[s * own : (s + 1) * own].astype(BF16)


def first_body(*refs, count, peers):
    gain, anomalies, means, sums = refs[:4]
    packets, blocks, (perturbed, root_out, inflation_out) = refs[4:7], refs[7 : 7 + peers], refs[7 + peers :]
    members = anomalies.shape[1]
    obs = packets[0].shape[1]
    folded = jnp.sum(sums[...], axis=0, keepdims=True)
    inflation = folded[:, 0:1] / folded[:, 1:2]
    inflation_out[0] = jnp.sum(inflation)
    root = jnp.sqrt(inflation)
    root_out[...] = jnp.broadcast_to(root, root_out.shape)
    for n, packet in enumerate(packets):
        innovation, error, spread, _ = scalar_rows(packet, members)
        bottom = jnp.where(error > 0.0, inflation * spread + error, 1.0)
        factor = jnp.where(error > 0.0, inflation / bottom, 0.0)
        scaled = packet[members : 2 * members].astype(F32)
        dev = packet[:members].astype(F32)
        perturbed[:, n * obs : (n + 1) * obs] = (
            factor * (innovation + scaled - root * dev)
        ).astype(BF16)
    for l in range(count):
        update(gain, anomalies, means, perturbed, root, blocks, l, l)


def first_updates(gain, anomalies, means, sums, packets, count, peers):
    _, members, width = anomalies.shape
    own = members // peers
    obs = packets[0].shape[1]
    out = pl.pallas_call(
        functools.partial(first_body, count=count, peers=peers),
        in_specs=[whole()] * 7,
        out_specs=[whole()] * (peers + 2) + [scalars()],
        out_shape=[shape_of((count, own, width))] * peers
        + [shape_of((members, 3 * obs)), shape_of((8, 128), F32), jax.ShapeDtypeStruct((1,), F32)],
        compiler_params=params(),
        name="first",
    )(*in_vmem((gain, anomalies, means, sums)), *in_vmem(packets))
    return out[:peers], out[peers], out[peers + 1], out[peers + 2]


def second_body(gain, anomalies, means, perturbed, root, *blocks, first):
    for l in range(blocks[0].shape[0]):
        update(gain, anomalies, means, perturbed, root[0:1, 0:1], blocks, first + l, l)


def second_updates(gain, anomalies, means, perturbed, root, first, peers):
    var_count, members, width = anomalies.shape
    own = members // peers
    return pl.pallas_call(
        functools.partial(second_body, first=first),
        in_specs=[whole()] * 5,
        out_specs=[whole()] * peers,
        out_shape=[shape_of((var_count - first, own, width))] * peers,
        compiler_params=params(),
        name="second",
    )(*in_vmem((gain, anomalies, means, perturbed, root)))


def place_body(me, *refs, first, peers):
    blocks, out, done = refs[:peers], refs[-2], refs[-1]
    count, _, width = blocks[0].shape
    copies = [
        pltpu.make_async_copy(
            blocks[s],
            out.at[first : first + count, :, pl.ds(tile_block(me[0], s, width), width)],
            done.at[s],
        )
        for s in range(peers)
    ]
    for copy in copies:
        copy.start()
    for copy in copies:
        copy.wait()


def place(me, blocks, first, var_count, before=None):
    peers = len(blocks)
    _, own, width = blocks[0].shape
    more = [] if before is None else [before]
    return pl.pallas_call(
        functools.partial(place_body, first=first, peers=peers),
        in_specs=[scalars()] + [anywhere()] * (peers + len(more)),
        out_specs=anywhere(),
        out_shape=pltpu.HBM((var_count, own, peers * width), BF16),
        scratch_shapes=[pltpu.SemaphoreType.DMA((peers,))],
        input_output_aliases={1 + peers: 0} if more else {},
        compiler_params=params(),
    )(me, *in_vmem(blocks), *more)


def swapped(value, axis, distance):
    pairs = [(i, i ^ distance) for i in range(lax.axis_size(axis))]
    return lax.ppermute(value, axis, pairs)


def exchanged(blocks, axis):
    return lax.all_to_all(blocks, axis, split_axis=0, concat_axis=0, tiled=True)


def traded(blocks, order):
    out = list(blocks)
    for s in order:
        out[s] = swapped(blocks[s], "member", s)
    return out


def shards(ensemble, obs_weights, obs_tiles, obs_values, obs_error, obs_noise):
    peers = lax.axis_size("member")
    regions = lax.axis_size("region")
    var_count, _, tile_count = ensemble.shape
    width = tile_count // peers
    me = lax.axis_index("member").astype(jnp.int32)[None]
    region = lax.axis_index("region").astype(jnp.int32)
    tiles, values, error = (a[None, :] for a in (obs_tiles, obs_values, obs_error))
    *blocks, partial = pack(me, ensemble, obs_weights, tiles, peers)
    other = swapped(partial, "depth", 1)
    states = traded(blocks, (1, 3, 2))
    joined = join(partial, other, obs_noise, error, peers)
    gathered = exchanged(joined, "member")
    packet, sums = stats(me, gathered, values, error, tiles, regions)
    near = swapped(packet, "region", 1)
    pairs = [(i, i + 1) for i in range(1, regions - 1, 2)]
    far = lax.ppermute(packet, "region", pairs + [(j, i) for i, j in pairs])
    all_sums = exchanged(sums, "region")
    side = 1 - 2 * (region % 2)
    offset = jnp.stack([me[0] * width, jnp.zeros_like(side), side, -side])
    packets = (packet, near, far)
    gain, anomalies, means = gains(offset, states, packets, tile_count)
    half = var_count // 2
    ready, perturbed, root, inflation = first_updates(
        gain, anomalies, means, all_sums, packets, half, peers
    )
    early = traded(ready, (1, 3, 2))
    ready = second_updates(gain, anomalies, means, perturbed, root, half, peers)
    late = traded(ready, (1, 3, 2))
    output = place(me, early, 0, var_count)
    output = place(me, late, half, var_count, output)
    return (output, inflation.reshape(()))


def solution(mesh):
    return jax.shard_map(
        shards,
        mesh=mesh,
        in_specs=(
            P("depth", "member", "region"),
            P("depth"),
            P("region"),
            P("region"),
            P("region"),
            P("member", "region"),
        ),
        out_specs=(P("depth", "member", "region"), P()),
        check_vma=False,
    )
```

```python
import functools

import jax
import jax.numpy as jnp
from jax import lax
from jax.experimental import pallas as pl
from jax.experimental.pallas import tpu as pltpu
from jax.sharding import PartitionSpec as P


RADIUS = 1024
F32 = jnp.float32
BF16 = jnp.bfloat16


def params(megabytes=12):
    return pltpu.CompilerParams(vmem_limit_bytes=megabytes * 2**20)


def whole():
    return pl.BlockSpec(memory_space=pltpu.VMEM)


def scalars():
    return pl.BlockSpec(memory_space=pltpu.SMEM)


def anywhere():
    return pl.BlockSpec(memory_space=pl.ANY)


def shape_of(shape, dtype=BF16):
    return pltpu.VMEM(shape, dtype)


def in_vmem(values):
    return [pltpu.with_memory_space_constraint(v, pltpu.VMEM) for v in values]


def split_rows(value):
    first = value.astype(BF16)
    rest = value - first.astype(F32)
    second = rest.astype(BF16)
    third = (rest - second.astype(F32)).astype(BF16)
    return [first, second, third]


def tile_block(me, s, width):
    return pl.multiple_of(jnp.bitwise_xor(me, s) * width, width)


def pack_body(me, weights, ensemble, tiles, *rest):
    *blocks, predicted, arrived = rest
    peers = len(blocks)
    var_count, _, width = blocks[0].shape
    starts = [tile_block(me[0], s, width) for s in range(peers)]
    loads = [
        pltpu.make_async_copy(
            ensemble.at[:, :, pl.ds(starts[s], width)], blocks[s], arrived.at[s]
        )
        for s in range(peers)
    ]
    for load in loads:
        load.start()
    rows = lax.broadcasted_iota(jnp.int32, (width, tiles.shape[1]), 0)
    total = jnp.zeros(predicted.shape, F32)
    for s in range(peers):
        chosen = jnp.where(tiles[...] - starts[s] == rows, 1.0, 0.0).astype(BF16)
        loads[s].wait()
        mixed = weights[0] * blocks[s][0].astype(F32)
        for l in range(1, var_count):
            mixed = mixed + weights[l] * blocks[s][l].astype(F32)
        high = mixed.astype(BF16)
        low = (mixed - high.astype(F32)).astype(BF16)
        total = total + jnp.dot(high, chosen, preferred_element_type=F32)
        total = total + jnp.dot(low, chosen, preferred_element_type=F32)
    predicted[...] = total.astype(BF16)


def pack(me, ensemble, weights, tiles, peers):
    var_count, own, tile_count = ensemble.shape
    width = tile_count // peers
    obs = tiles.shape[1]
    return pl.pallas_call(
        pack_body,
        in_specs=[scalars(), scalars(), anywhere(), whole()],
        out_specs=[whole()] * (peers + 1),
        out_shape=[shape_of((var_count, own, width))] * peers + [shape_of((own, obs))],
        scratch_shapes=[pltpu.SemaphoreType.DMA((peers,))],
        compiler_params=params(),
        name="pack",
    )(me, weights, pltpu.with_memory_space_constraint(ensemble, pltpu.HBM), tiles)


def scale_body(noise, error, out):
    out[...] = (jnp.sqrt(error[...]) * noise[...]).astype(BF16)


def scale(noise, error):
    return pl.pallas_call(
        scale_body,
        in_specs=[whole()] * 2,
        out_specs=whole(),
        out_shape=shape_of(noise.shape),
        compiler_params=params(),
        name="scale",
    )(noise, error)


def join_body(mine, other, out):
    predicted = (mine[...].astype(F32) + other[...].astype(F32)).astype(BF16)
    for j in range(out.shape[0]):
        out[j] = predicted


def join(mine, other, peers):
    return pl.pallas_call(
        join_body,
        in_specs=[whole()] * 2,
        out_specs=whole(),
        out_shape=shape_of((peers, *mine.shape)),
        compiler_params=params(),
        name="join",
    )(mine, other)


def stats_body(me, gathered, values, error, tiles, *refs):
    peers, own, obs = gathered.shape
    noises, (packet, sums) = refs[:peers], refs[peers:]
    members = peers * own
    total = jnp.zeros((1, obs), F32)
    for j in range(peers):
        total = total + jnp.sum(gathered[j].astype(F32), axis=0, keepdims=True)
    mean = total / members
    square = jnp.zeros((1, obs), F32)
    for j in range(peers):
        dev = gathered[j].astype(F32) - mean
        square = square + jnp.sum(dev * dev, axis=0, keepdims=True)
    for s in range(peers):
        dev = gathered[jnp.bitwise_xor(me[0], s)].astype(F32) - mean
        packet[s * own : (s + 1) * own] = dev.astype(BF16)
        packet[members + s * own : members + (s + 1) * own] = noises[s][...]
    spread = square / (members - 1)
    innovation = values[...] - mean
    place = tiles[...]
    rows = split_rows(innovation) + split_rows(error[...]) + split_rows(spread)
    rows += [(place // 32).astype(F32).astype(BF16), (place % 32).astype(F32).astype(BF16)]
    rows += [jnp.zeros((1, obs), BF16)] * (16 - len(rows))
    packet[2 * members :] = jnp.concatenate(rows, axis=0)
    above = jnp.sum(innovation * innovation)
    below = jnp.sum(spread + error[...])
    lane = lax.broadcasted_iota(jnp.int32, sums.shape, 1)
    sums[...] = jnp.where(lane == 0, above, jnp.where(lane == 1, below, 0.0))


def stats(me, gathered, values, error, tiles, noises, regions):
    peers, own, obs = gathered.shape
    return pl.pallas_call(
        stats_body,
        in_specs=[scalars()] + [whole()] * (4 + peers),
        out_specs=[whole(), whole()],
        out_shape=[shape_of((2 * peers * own + 16, obs)), shape_of((regions, 128), F32)],
        compiler_params=params(),
        name="stats",
    )(me, gathered, values, error, tiles, *noises)


def scalar_rows(packet, members):
    rows = packet[2 * members :].astype(F32)
    innovation = rows[0:1] + rows[1:2] + rows[2:3]
    error = rows[3:4] + rows[4:5] + rows[5:6]
    spread = rows[6:7] + rows[7:8] + rows[8:9]
    return innovation, error, spread, rows[9:10] * 32.0 + rows[10:11]


def update(state, anom_t, perturbed, taper, root, anomalies, gain, blocks, at):
    own = blocks[0].shape[1]
    members = own * len(blocks)
    parts = [part.astype(F32) for part in state]
    mean = sum(jnp.sum(part, axis=0, keepdims=True) for part in parts) / members
    for s, part in enumerate(parts):
        anomalies[s * own : (s + 1) * own] = (part - mean).astype(BF16)
    obs = taper.shape[0]
    step = obs // 3
    for k in range(0, obs, step):
        covariance = jnp.dot(anom_t[k : k + step], anomalies[...], preferred_element_type=F32)
        gain[k : k + step] = (covariance * taper[k : k + step]).astype(BF16)
    increment = jnp.dot(perturbed[...], gain[...], preferred_element_type=F32)
    result = mean + root * anomalies[...].astype(F32) + increment
    for s, block in enumerate(blocks):
        block[at] = result[s * own : (s + 1) * own].astype(BF16)


def first_body(offset, *refs, tile_count, peers):
    far_states, far_packets, sums = refs[:peers], refs[peers : peers + 3], refs[peers + 3]
    refs = refs[peers + 4 :]
    blocks, (anom_t, perturbed, taper, root_out, inflation_out) = refs[:peers], refs[peers : peers + 5]
    states, packets, anomalies, gain, arrived = refs[peers + 5 :]
    count, own, width = blocks[0].shape
    members = peers * own
    obs = far_packets[0].shape[1]
    loads = [
        pltpu.make_async_copy(far_packets[n], packets.at[n], arrived.at[n]) for n in range(3)
    ]
    loads += [
        pltpu.make_async_copy(far_states[s].at[:count], states.at[s], arrived.at[3 + s])
        for s in range(peers)
    ]
    for load in loads:
        load.start()
    folded = jnp.sum(sums[...], axis=0, keepdims=True)
    inflation = folded[:, 0:1] / folded[:, 1:2]
    inflation_out[0] = jnp.sum(inflation)
    root = jnp.sqrt(inflation)
    root_out[...] = jnp.broadcast_to(root, root_out.shape)
    tile = (offset[0] + lax.broadcasted_iota(jnp.int32, (1, width), 1)).astype(F32)
    for n in range(3):
        loads[n].wait()
        packet = packets.at[n]
        dev = packet[:members]
        anom_t[n * obs : (n + 1) * obs] = dev.T
        innovation, error, spread, place = scalar_rows(packet, members)
        place = place + (offset[1 + n] * tile_count).astype(F32)
        bottom = jnp.where(error > 0.0, inflation * spread + error, 1.0)
        factor = jnp.where(error > 0.0, inflation / bottom, 0.0) / (members - 1)
        column = jnp.concatenate([place, factor, jnp.zeros((6, obs), F32)], axis=0).T
        near = jnp.maximum(0.0, 1.0 - jnp.abs(tile - column[:, 0:1]) / RADIUS)
        taper[n * obs : (n + 1) * obs] = near * near * column[:, 1:2]
        scaled = packet[members : 2 * members].astype(F32)
        perturbed[:, n * obs : (n + 1) * obs] = (
            innovation + scaled - root * dev.astype(F32)
        ).astype(BF16)
    for load in loads[3:]:
        load.wait()
    for l in range(count):
        update(
            [states[s, l] for s in range(peers)],
            anom_t, perturbed, taper, root, anomalies.at[l], gain.at[l], blocks, l,
        )


def first_updates(offset, states, packets, sums, count, tile_count):
    _, own, width = states[0].shape
    peers = len(states)
    members = own * peers
    rows, obs = packets[0].shape
    out = pl.pallas_call(
        functools.partial(first_body, tile_count=tile_count, peers=peers),
        in_specs=[scalars()] + [anywhere()] * (peers + 3) + [whole()],
        out_specs=[whole()] * (peers + 4) + [scalars()],
        out_shape=[shape_of((count, own, width))] * peers
        + [
            shape_of((3 * obs, members)),
            shape_of((members, 3 * obs)),
            shape_of((3 * obs, width), F32),
            shape_of((8, 128), F32),
            jax.ShapeDtypeStruct((1,), F32),
        ],
        scratch_shapes=[
            pltpu.VMEM((peers, count, own, width), BF16),
            pltpu.VMEM((3, rows, obs), BF16),
            pltpu.VMEM((count, members, width), BF16),
            pltpu.VMEM((count, 3 * obs, width), BF16),
            pltpu.SemaphoreType.DMA((3 + peers,)),
        ],
        compiler_params=params(16),
        name="first",
    )(offset, *states, *packets, sums)
    return out[:peers], out[peers : peers + 4], out[peers + 4]


def second_body(*refs, first, peers):
    far_states, (anom_t, perturbed, taper, root) = refs[:peers], refs[peers : peers + 4]
    blocks = refs[peers + 4 : 2 * peers + 4]
    states, anomalies, gain, arrived = refs[2 * peers + 4 :]
    count = blocks[0].shape[0]
    loads = [
        pltpu.make_async_copy(far_states[s].at[first:], states.at[s], arrived.at[s])
        for s in range(peers)
    ]
    for load in loads:
        load.start()
    for load in loads:
        load.wait()
    for l in range(count):
        update(
            [states[s, l] for s in range(peers)],
            anom_t, perturbed, taper, root[0:1, 0:1], anomalies.at[l], gain.at[l], blocks, l,
        )


def second_updates(states, shared, first):
    var_count, own, width = states[0].shape
    peers = len(states)
    members = own * peers
    count = var_count - first
    obs = shared[0].shape[0]
    return pl.pallas_call(
        functools.partial(second_body, first=first, peers=peers),
        in_specs=[anywhere()] * peers + [whole()] * 4,
        out_specs=[whole()] * peers,
        out_shape=[shape_of((count, own, width))] * peers,
        scratch_shapes=[
            pltpu.VMEM((peers, count, own, width), BF16),
            pltpu.VMEM((count, members, width), BF16),
            pltpu.VMEM((count, obs, width), BF16),
            pltpu.SemaphoreType.DMA((peers,)),
        ],
        compiler_params=params(),
        name="second",
    )(*states, *in_vmem(shared))


def place_body(me, *refs, first, peers):
    blocks, out, done = refs[:peers], refs[-2], refs[-1]
    count, _, width = blocks[0].shape
    copies = [
        pltpu.make_async_copy(
            blocks[s],
            out.at[first : first + count, :, pl.ds(tile_block(me[0], s, width), width)],
            done.at[s],
        )
        for s in range(peers)
    ]
    for copy in copies:
        copy.start()
    for copy in copies:
        copy.wait()


def place(me, blocks, first, var_count, before=None):
    peers = len(blocks)
    _, own, width = blocks[0].shape
    more = [] if before is None else [before]
    return pl.pallas_call(
        functools.partial(place_body, first=first, peers=peers),
        in_specs=[scalars()] + [anywhere()] * (peers + len(more)),
        out_specs=anywhere(),
        out_shape=pltpu.HBM((var_count, own, peers * width), BF16),
        scratch_shapes=[pltpu.SemaphoreType.DMA((peers,))],
        input_output_aliases={1 + peers: 0} if more else {},
        compiler_params=params(),
    )(me, *in_vmem(blocks), *more)


def swapped(value, axis, distance):
    pairs = [(i, i ^ distance) for i in range(lax.axis_size(axis))]
    return lax.ppermute(value, axis, pairs)


def exchanged(blocks, axis):
    return lax.all_to_all(blocks, axis, split_axis=0, concat_axis=0, tiled=True)


def traded(blocks, order):
    out = list(blocks)
    for s in order:
        out[s] = swapped(blocks[s], "member", s)
    return out


def shards(ensemble, obs_weights, obs_tiles, obs_values, obs_error, obs_noise):
    peers = lax.axis_size("member")
    regions = lax.axis_size("region")
    var_count, _, tile_count = ensemble.shape
    width = tile_count // peers
    me = lax.axis_index("member").astype(jnp.int32)[None]
    region = lax.axis_index("region").astype(jnp.int32)
    tiles, values, error = (a[None, :] for a in (obs_tiles, obs_values, obs_error))
    *blocks, partial = pack(me, ensemble, obs_weights, tiles, peers)
    other = swapped(partial, "depth", 1)
    noises = traded([scale(obs_noise, error)] * peers, (1, 3, 2))
    states = traded(blocks, (1, 3, 2))
    joined = join(partial, other, peers)
    gathered = exchanged(joined, "member")
    packet, sums = stats(me, gathered, values, error, tiles, noises, regions)
    near = swapped(packet, "region", 1)
    pairs = [(i, i + 1) for i in range(1, regions - 1, 2)]
    far = lax.ppermute(packet, "region", pairs + [(j, i) for i, j in pairs])
    all_sums = exchanged(sums, "region")
    side = 1 - 2 * (region % 2)
    offset = jnp.stack([me[0] * width, jnp.zeros_like(side), side, -side])
    half = var_count // 2
    ready, shared, inflation = first_updates(
        offset, states, (packet, near, far), all_sums, half, tile_count
    )
    early = traded(ready, (1, 3, 2))
    ready = second_updates(states, shared, half)
    late = traded(ready, (1, 3, 2))
    output = place(me, early, 0, var_count)
    output = place(me, late, half, var_count, output)
    return (output, inflation.reshape(()))


def solution(mesh):
    return jax.shard_map(
        shards,
        mesh=mesh,
        in_specs=(
            P("depth", "member", "region"),
            P("depth"),
            P("region"),
            P("region"),
            P("region"),
            P("member", "region"),
        ),
        out_specs=(P("depth", "member", "region"), P()),
        check_vma=False,
    )
```

```python
import functools

import jax
import jax.numpy as jnp
from jax import lax
from jax.experimental import pallas as pl
from jax.experimental.pallas import tpu as pltpu
from jax.sharding import PartitionSpec as P


RADIUS = 1024
F32 = jnp.float32
BF16 = jnp.bfloat16


def params(megabytes=12):
    return pltpu.CompilerParams(vmem_limit_bytes=megabytes * 2**20)


def whole():
    return pl.BlockSpec(memory_space=pltpu.VMEM)


def scalars():
    return pl.BlockSpec(memory_space=pltpu.SMEM)


def anywhere():
    return pl.BlockSpec(memory_space=pl.ANY)


def shape_of(shape, dtype=BF16):
    return pltpu.VMEM(shape, dtype)


def in_vmem(values):
    return [pltpu.with_memory_space_constraint(v, pltpu.VMEM) for v in values]


def in_hbm(value):
    return pltpu.with_memory_space_constraint(value, pltpu.HBM)


def split_rows(value):
    first = value.astype(BF16)
    rest = value - first.astype(F32)
    second = rest.astype(BF16)
    third = (rest - second.astype(F32)).astype(BF16)
    return [first, second, third]


def tile_block(me, s, width):
    return pl.multiple_of(jnp.bitwise_xor(me, s) * width, width)


def pack_body(me, far_weights, ensemble, tiles, *rest):
    *blocks, predicted, weights, buffer, arrived, left = rest
    peers, var_count, _, width = buffer.shape
    starts = [tile_block(me[0], s, width) for s in range(peers)]
    loads = [
        pltpu.make_async_copy(
            ensemble.at[:, :, pl.ds(starts[s], width)], buffer.at[s], arrived.at[s]
        )
        for s in range(peers)
    ]
    stores = [pltpu.make_async_copy(buffer.at[s], blocks[s], left.at[s]) for s in range(peers)]
    light = pltpu.make_async_copy(far_weights, weights, arrived.at[peers])
    light.start()
    for load in loads:
        load.start()
    light.wait()
    rows = lax.broadcasted_iota(jnp.int32, (width, tiles.shape[1]), 0)
    total = jnp.zeros(predicted.shape, F32)
    for s in range(peers):
        chosen = jnp.where(tiles[...] - starts[s] == rows, 1.0, 0.0).astype(BF16)
        loads[s].wait()
        stores[s].start()
        mixed = weights[0] * buffer[s, 0].astype(F32)
        for l in range(1, var_count):
            mixed = mixed + weights[l] * buffer[s, l].astype(F32)
        high = mixed.astype(BF16)
        low = (mixed - high.astype(F32)).astype(BF16)
        total = total + jnp.dot(high, chosen, preferred_element_type=F32)
        total = total + jnp.dot(low, chosen, preferred_element_type=F32)
    predicted[...] = total.astype(BF16)
    for store in stores:
        store.wait()


def pack(me, ensemble, weights, tiles, peers):
    var_count, own, tile_count = ensemble.shape
    width = tile_count // peers
    obs = tiles.shape[1]
    return pl.pallas_call(
        pack_body,
        in_specs=[scalars(), anywhere(), anywhere(), whole()],
        out_specs=[anywhere()] * peers + [whole()],
        out_shape=[pltpu.HBM((var_count, own, width), BF16)] * peers + [shape_of((own, obs))],
        scratch_shapes=[
            pltpu.SMEM((var_count,), F32),
            pltpu.VMEM((peers, var_count, own, width), BF16),
            pltpu.SemaphoreType.DMA((peers + 1,)),
            pltpu.SemaphoreType.DMA((peers,)),
        ],
        compiler_params=params(),
        name="pack",
    )(me, in_hbm(weights), in_hbm(ensemble), tiles)


def scale_body(noise, error, out):
    scaled = (jnp.sqrt(error[...]) * noise[...]).astype(BF16)
    for j in range(out.shape[0]):
        out[j] = scaled


def scale(noise, error, peers):
    return pl.pallas_call(
        scale_body,
        in_specs=[whole()] * 2,
        out_specs=whole(),
        out_shape=shape_of((peers, *noise.shape)),
        compiler_params=params(),
        name="scale",
    )(noise, error)


def join_body(mine, other, out):
    out[...] = (mine[...].astype(F32) + other[...].astype(F32)).astype(BF16)


def join(mine, other):
    return pl.pallas_call(
        join_body,
        in_specs=[whole()] * 2,
        out_specs=whole(),
        out_shape=shape_of(mine.shape),
        compiler_params=params(),
        name="join",
    )(mine, other)


def stats_body(me, values, error, tiles, *refs):
    *gathered, packet, sums, ordered = refs
    peers = len(gathered)
    own, obs = gathered[0].shape
    members = peers * own
    for s in range(peers):
        part = jnp.sum(gathered[s][...].astype(F32), axis=0, keepdims=True)
        ordered[jnp.bitwise_xor(me[0], s)] = jnp.broadcast_to(part, ordered.shape[1:])
    mean = (ordered[0] + ordered[1] + ordered[2] + ordered[3])[0:1] / members
    for s in range(peers):
        dev = gathered[s][...].astype(F32) - mean
        packet[s * own : (s + 1) * own] = dev.astype(BF16)
        part = jnp.sum(dev * dev, axis=0, keepdims=True)
        ordered[jnp.bitwise_xor(me[0], s)] = jnp.broadcast_to(part, ordered.shape[1:])
    spread = (ordered[0] + ordered[1] + ordered[2] + ordered[3])[0:1] / (members - 1)
    innovation = values[...] - mean
    place = tiles[...]
    rows = split_rows(innovation) + split_rows(error[...]) + split_rows(spread)
    rows += [(place // 32).astype(F32).astype(BF16), (place % 32).astype(F32).astype(BF16)]
    rows += [jnp.zeros((1, obs), BF16)] * (16 - len(rows))
    packet[members:] = jnp.concatenate(rows, axis=0)
    above = jnp.sum(innovation * innovation)
    below = jnp.sum(spread + error[...])
    lane = lax.broadcasted_iota(jnp.int32, sums.shape, 1)
    sums[...] = jnp.where(lane == 0, above, jnp.where(lane == 1, below, 0.0))


def stats(me, gathered, values, error, tiles, regions):
    peers = len(gathered)
    own, obs = gathered[0].shape
    return pl.pallas_call(
        stats_body,
        in_specs=[scalars()] + [whole()] * (3 + peers),
        out_specs=[whole(), whole()],
        out_shape=[shape_of((peers * own + 16, obs)), shape_of((regions, 128), F32)],
        scratch_shapes=[pltpu.VMEM((peers, 8, obs), F32)],
        compiler_params=params(),
        name="stats",
    )(me, values, error, tiles, *gathered)


def scalar_rows(packet, members):
    rows = packet[members:].astype(F32)
    innovation = rows[0:1] + rows[1:2] + rows[2:3]
    error = rows[3:4] + rows[4:5] + rows[5:6]
    spread = rows[6:7] + rows[7:8] + rows[8:9]
    return innovation, error, spread, rows[9:10] * 32.0 + rows[10:11]


def gains(state, anom_t, taper, means, anomalies, gain):
    own = state[0].shape[0]
    parts = [part.astype(F32) for part in state]
    mean = sum(jnp.sum(part, axis=0, keepdims=True) for part in parts) / (own * len(parts))
    means[...] = jnp.broadcast_to(mean, means.shape)
    for s, part in enumerate(parts):
        anomalies[s * own : (s + 1) * own] = (part - mean).astype(BF16)
    obs = taper.shape[0]
    step = obs // 3
    for k in range(0, obs, step):
        covariance = jnp.dot(anom_t[k : k + step], anomalies[...], preferred_element_type=F32)
        gain[k : k + step] = (covariance * taper[k : k + step]).astype(BF16)


def posterior(gain, means, anomalies, perturbed, root, blocks, at):
    own = blocks[0].shape[1]
    increment = jnp.dot(perturbed[...], gain[...], preferred_element_type=F32)
    result = means[0:1] + root * anomalies[...].astype(F32) + increment
    for s, block in enumerate(blocks):
        block[at] = result[s * own : (s + 1) * own].astype(BF16)


def prepare_body(offset, *refs, tile_count):
    *far_packets, anom_t, taper, packets, arrived = refs
    members = anom_t.shape[1]
    obs = packets.shape[2]
    loads = [pltpu.make_async_copy(far_packets[n], packets.at[n], arrived.at[n]) for n in range(3)]
    for load in loads:
        load.start()
    tile = (offset[0] + lax.broadcasted_iota(jnp.int32, (1, taper.shape[1]), 1)).astype(F32)
    for n in range(3):
        loads[n].wait()
        packet = packets.at[n]
        anom_t[n * obs : (n + 1) * obs] = packet[:members].T
        place = scalar_rows(packet, members)[3] + (offset[1 + n] * tile_count).astype(F32)
        column = jnp.broadcast_to(place, (8, obs)).T[:, 0:1]
        near = jnp.maximum(0.0, 1.0 - jnp.abs(tile - column) / RADIUS)
        taper[n * obs : (n + 1) * obs] = near * near / (members - 1)


def prepare(offset, packets, width, tile_count):
    rows, obs = packets[0].shape
    members = rows - 16
    return pl.pallas_call(
        functools.partial(prepare_body, tile_count=tile_count),
        in_specs=[scalars()] + [anywhere()] * 3,
        out_specs=[whole()] * 2,
        out_shape=[shape_of((3 * obs, members)), shape_of((3 * obs, width), F32)],
        scratch_shapes=[pltpu.VMEM((3, rows, obs), BF16), pltpu.SemaphoreType.DMA((3,))],
        compiler_params=params(),
        name="prepare",
    )(offset, *map(in_hbm, packets))


def first_body(me, *refs, peers):
    far_states, far_packets = refs[:peers], refs[peers : peers + 3]
    far_noises, (sums, anom_t, taper) = refs[peers + 3 : peers + 6], refs[peers + 6 : peers + 9]
    refs = refs[peers + 9 :]
    blocks, (perturbed, root_out, inflation_out) = refs[:peers], refs[peers : peers + 3]
    states, packets, noises, means, anomalies, gain, arrived = refs[peers + 3 :]
    count, own, _ = blocks[0].shape
    members = peers * own
    obs = packets.shape[2]
    loads = [
        pltpu.make_async_copy(far_states[s].at[:count], states.at[s], arrived.at[s])
        for s in range(peers)
    ]
    late = [
        pltpu.make_async_copy(source[n], target.at[n], arrived.at[peers + 3 * i + n])
        for i, (source, target) in enumerate(((far_packets, packets), (far_noises, noises)))
        for n in range(3)
    ]
    for load in loads + late:
        load.start()
    for load in loads:
        load.wait()
    for l in range(count):
        state = [states[s, l] for s in range(peers)]
        gains(state, anom_t, taper, means.at[l], anomalies.at[l], gain.at[l])
    for load in late:
        load.wait()
    folded = jnp.sum(sums[...], axis=0, keepdims=True)
    inflation = folded[:, 0:1] / folded[:, 1:2]
    inflation_out[0] = jnp.sum(inflation)
    root = jnp.sqrt(inflation)
    root_out[...] = jnp.broadcast_to(root, root_out.shape)
    for n in range(3):
        innovation, error, spread, _ = scalar_rows(packets.at[n], members)
        bottom = jnp.where(error > 0.0, inflation * spread + error, 1.0)
        factor = jnp.where(error > 0.0, inflation / bottom, 0.0)
        for s in range(peers):
            rows = slice(s * own, (s + 1) * own)
            noise = noises[n, jnp.bitwise_xor(me[0], s)].astype(F32)
            dev = packets[n, rows].astype(F32)
            perturbed[rows, n * obs : (n + 1) * obs] = (
                factor * (innovation + noise - root * dev)
            ).astype(BF16)
    for l in range(count):
        posterior(gain.at[l], means.at[l], anomalies.at[l], perturbed, root, blocks, l)


def working(count, members, obs, width):
    return [
        pltpu.VMEM((count, 8, width), F32),
        pltpu.VMEM((count, members, width), BF16),
        pltpu.VMEM((count, obs, width), BF16),
    ]


def first_updates(me, states, packets, noises, sums, anom_t, taper, count):
    _, own, width = states[0].shape
    peers = len(states)
    members = own * peers
    rows, obs = packets[0].shape
    out = pl.pallas_call(
        functools.partial(first_body, peers=peers),
        in_specs=[scalars()] + [anywhere()] * (peers + 6) + [whole()] * 3,
        out_specs=[whole()] * (peers + 2) + [scalars()],
        out_shape=[shape_of((count, own, width))] * peers
        + [
            shape_of((members, 3 * obs)),
            shape_of((8, 128), F32),
            jax.ShapeDtypeStruct((1,), F32),
        ],
        scratch_shapes=[
            pltpu.VMEM((peers, count, own, width), BF16),
            pltpu.VMEM((3, rows, obs), BF16),
            pltpu.VMEM((3, peers, own, obs), BF16),
            *working(count, members, 3 * obs, width),
            pltpu.SemaphoreType.DMA((peers + 6,)),
        ],
        compiler_params=params(16),
        name="first",
    )(me, *map(in_hbm, (*states, *packets, *noises)), *in_vmem((sums, anom_t, taper)))
    return out[:peers], out[peers], out[peers + 1], out[peers + 2]


def second_body(*refs, first, peers):
    states, (anom_t, perturbed, taper, root) = refs[:peers], refs[peers : peers + 4]
    blocks = refs[peers + 4 : 2 * peers + 4]
    means, anomalies, gain = refs[2 * peers + 4 :]
    count = blocks[0].shape[0]
    for l in range(count):
        state = [states[s][first + l] for s in range(peers)]
        gains(state, anom_t, taper, means.at[l], anomalies.at[l], gain.at[l])
    for l in range(count):
        posterior(gain.at[l], means.at[l], anomalies.at[l], perturbed, root[0:1, 0:1], blocks, l)


def second_updates(states, anom_t, perturbed, taper, root, first):
    var_count, own, width = states[0].shape
    peers = len(states)
    members = own * peers
    count = var_count - first
    return pl.pallas_call(
        functools.partial(second_body, first=first, peers=peers),
        in_specs=[whole()] * (peers + 4),
        out_specs=[whole()] * peers,
        out_shape=[shape_of((count, own, width))] * peers,
        scratch_shapes=working(count, members, anom_t.shape[0], width),
        compiler_params=params(),
        name="second",
    )(*in_vmem((*states, anom_t, perturbed, taper, root)))


def place_body(me, *refs, first, peers):
    blocks, out, done = refs[:peers], refs[-2], refs[-1]
    count, _, width = blocks[0].shape
    copies = [
        pltpu.make_async_copy(
            blocks[s],
            out.at[first : first + count, :, pl.ds(tile_block(me[0], s, width), width)],
            done.at[s],
        )
        for s in range(peers)
    ]
    for copy in copies:
        copy.start()
    for copy in copies:
        copy.wait()


def place(me, blocks, first, var_count, before=None):
    peers = len(blocks)
    _, own, width = blocks[0].shape
    more = [] if before is None else [before]
    return pl.pallas_call(
        functools.partial(place_body, first=first, peers=peers),
        in_specs=[scalars()] + [anywhere()] * (peers + len(more)),
        out_specs=anywhere(),
        out_shape=pltpu.HBM((var_count, own, peers * width), BF16),
        scratch_shapes=[pltpu.SemaphoreType.DMA((peers,))],
        input_output_aliases={1 + peers: 0} if more else {},
        compiler_params=params(),
    )(me, *in_vmem(blocks), *more)


def swapped(value, axis, distance):
    pairs = [(i, i ^ distance) for i in range(lax.axis_size(axis))]
    return lax.ppermute(value, axis, pairs)


def exchanged(blocks, axis):
    return lax.all_to_all(blocks, axis, split_axis=0, concat_axis=0, tiled=True)


def traded(blocks, order):
    out = list(blocks)
    for s in order:
        out[s] = swapped(blocks[s], "member", s)
    return out


def shards(ensemble, obs_weights, obs_tiles, obs_values, obs_error, obs_noise):
    peers = lax.axis_size("member")
    regions = lax.axis_size("region")
    var_count, _, tile_count = ensemble.shape
    width = tile_count // peers
    me = lax.axis_index("member").astype(jnp.int32)[None]
    region = lax.axis_index("region").astype(jnp.int32)
    tiles, values, error = (a[None, :] for a in (obs_tiles, obs_values, obs_error))
    *blocks, partial = pack(me, ensemble, obs_weights, tiles, peers)
    other = swapped(partial, "depth", 1)
    noise = exchanged(scale(obs_noise, error, peers), "member")
    predicted = traded([join(partial, other)] * peers, (1, 3, 2))
    pairs = [(i, i + 1) for i in range(1, regions - 1, 2)]
    pairs += [(j, i) for i, j in pairs]
    near_noise = swapped(noise, "region", 1)
    far_noise = lax.ppermute(noise, "region", pairs)
    packet, sums = stats(me, predicted, values, error, tiles, regions)
    near = swapped(packet, "region", 1)
    far = lax.ppermute(packet, "region", pairs)
    states = traded(blocks, (1, 3, 2))
    all_sums = exchanged(sums, "region")
    side = 1 - 2 * (region % 2)
    offset = jnp.stack([me[0] * width, jnp.zeros_like(side), side, -side])
    packets = (packet, near, far)
    anom_t, taper = prepare(offset, packets, width, tile_count)
    half = (var_count + 1) // 2
    ready, perturbed, root, inflation = first_updates(
        me, states, packets, (noise, near_noise, far_noise), all_sums, anom_t, taper, half
    )
    early = traded(ready, (1, 3, 2))
    ready = second_updates(states, anom_t, perturbed, taper, root, half)
    late = traded(ready, (1, 3, 2))
    output = place(me, early, 0, var_count)
    output = place(me, late, half, var_count, output)
    return (output, inflation.reshape(()))


def solution(mesh):
    return jax.shard_map(
        shards,
        mesh=mesh,
        in_specs=(
            P("depth", "member", "region"),
            P("depth"),
            P("region"),
            P("region"),
            P("region"),
            P("member", "region"),
        ),
        out_specs=(P("depth", "member", "region"), P()),
        check_vma=False,
    )
```

```python
import functools

import jax
import jax.numpy as jnp
from jax import lax
from jax.experimental import pallas as pl
from jax.experimental.pallas import tpu as pltpu
from jax.sharding import PartitionSpec as P


RADIUS = 1024
F32 = jnp.float32
BF16 = jnp.bfloat16


def params(megabytes=12):
    return pltpu.CompilerParams(vmem_limit_bytes=megabytes * 2**20)


def whole():
    return pl.BlockSpec(memory_space=pltpu.VMEM)


def scalars():
    return pl.BlockSpec(memory_space=pltpu.SMEM)


def anywhere():
    return pl.BlockSpec(memory_space=pl.ANY)


def shape_of(shape, dtype=BF16):
    return pltpu.VMEM(shape, dtype)


def in_vmem(values):
    return [pltpu.with_memory_space_constraint(v, pltpu.VMEM) for v in values]


def in_hbm(value):
    return pltpu.with_memory_space_constraint(value, pltpu.HBM)


def split_rows(value):
    first = value.astype(BF16)
    rest = value - first.astype(F32)
    second = rest.astype(BF16)
    third = (rest - second.astype(F32)).astype(BF16)
    return [first, second, third]


def tile_block(me, s, width):
    return pl.multiple_of(jnp.bitwise_xor(me, s) * width, width)


def pack_body(me, far_weights, ensemble, far_tiles, *rest):
    *blocks, predicted, weights, tiles, buffer, arrived, left = rest
    peers, var_count, _, width = buffer.shape
    starts = [tile_block(me[0], s, width) for s in range(peers)]
    loads = [
        pltpu.make_async_copy(
            ensemble.at[:, :, pl.ds(starts[s], width)], buffer.at[s], arrived.at[s]
        )
        for s in range(peers)
    ]
    stores = [pltpu.make_async_copy(buffer.at[s], blocks[s], left.at[s]) for s in range(peers)]
    light = [
        pltpu.make_async_copy(far_weights, weights, arrived.at[peers]),
        pltpu.make_async_copy(far_tiles, tiles, arrived.at[peers + 1]),
    ]
    for load in light + loads:
        load.start()
    for load in light:
        load.wait()
    rows = lax.broadcasted_iota(jnp.int32, (width, tiles.shape[1]), 0)
    total = jnp.zeros(predicted.shape, F32)
    for s in range(peers):
        chosen = jnp.where(tiles[...] - starts[s] == rows, 1.0, 0.0).astype(BF16)
        loads[s].wait()
        stores[s].start()
        mixed = weights[0] * buffer[s, 0].astype(F32)
        for l in range(1, var_count):
            mixed = mixed + weights[l] * buffer[s, l].astype(F32)
        high = mixed.astype(BF16)
        low = (mixed - high.astype(F32)).astype(BF16)
        total = total + jnp.dot(high, chosen, preferred_element_type=F32)
        total = total + jnp.dot(low, chosen, preferred_element_type=F32)
    predicted[...] = total.astype(BF16)
    for store in stores:
        store.wait()


def pack(me, ensemble, weights, tiles, peers):
    var_count, own, tile_count = ensemble.shape
    width = tile_count // peers
    obs = tiles.shape[1]
    return pl.pallas_call(
        pack_body,
        in_specs=[scalars()] + [anywhere()] * 3,
        out_specs=[anywhere()] * peers + [whole()],
        out_shape=[pltpu.HBM((var_count, own, width), BF16)] * peers + [shape_of((own, obs))],
        scratch_shapes=[
            pltpu.SMEM((var_count,), F32),
            pltpu.VMEM((1, obs), jnp.int32),
            pltpu.VMEM((peers, var_count, own, width), BF16),
            pltpu.SemaphoreType.DMA((peers + 2,)),
            pltpu.SemaphoreType.DMA((peers,)),
        ],
        compiler_params=params(),
        name="pack",
    )(me, in_hbm(weights), in_hbm(ensemble), in_hbm(tiles))


def scale_body(noise, error, out):
    out[...] = (jnp.sqrt(error[...]) * noise[...]).astype(BF16)


def scale(noise, error):
    return pl.pallas_call(
        scale_body,
        in_specs=[whole()] * 2,
        out_specs=whole(),
        out_shape=shape_of(noise.shape),
        compiler_params=params(),
        name="scale",
    )(noise, error)


def join_noise_body(*refs):
    *parts, out = refs
    own = parts[0].shape[0]
    for s, part in enumerate(parts):
        out[s * own : (s + 1) * own] = part[...]


def join_noise(parts):
    own, obs = parts[0].shape
    return pl.pallas_call(
        join_noise_body,
        in_specs=[whole()] * len(parts),
        out_specs=whole(),
        out_shape=shape_of((len(parts) * own, obs)),
        compiler_params=params(),
        name="joinnoise",
    )(*parts)


def join_body(mine, other, out):
    out[...] = (mine[...].astype(F32) + other[...].astype(F32)).astype(BF16)


def join(mine, other):
    return pl.pallas_call(
        join_body,
        in_specs=[whole()] * 2,
        out_specs=whole(),
        out_shape=shape_of(mine.shape),
        compiler_params=params(),
        name="join",
    )(mine, other)


def stats_body(me, values, error, tiles, *refs):
    *gathered, packet, sums, ordered = refs
    peers = len(gathered)
    own, obs = gathered[0].shape
    members = peers * own
    for s in range(peers):
        part = jnp.sum(gathered[s][...].astype(F32), axis=0, keepdims=True)
        ordered[jnp.bitwise_xor(me[0], s)] = jnp.broadcast_to(part, ordered.shape[1:])
    mean = (ordered[0] + ordered[1] + ordered[2] + ordered[3])[0:1] / members
    for s in range(peers):
        dev = gathered[s][...].astype(F32) - mean
        packet[s * own : (s + 1) * own] = dev.astype(BF16)
        part = jnp.sum(dev * dev, axis=0, keepdims=True)
        ordered[jnp.bitwise_xor(me[0], s)] = jnp.broadcast_to(part, ordered.shape[1:])
    spread = (ordered[0] + ordered[1] + ordered[2] + ordered[3])[0:1] / (members - 1)
    innovation = values[...] - mean
    place = tiles[...]
    rows = split_rows(innovation) + split_rows(error[...]) + split_rows(spread)
    rows += [(place // 32).astype(F32).astype(BF16), (place % 32).astype(F32).astype(BF16)]
    rows += [jnp.zeros((1, obs), BF16)] * (16 - len(rows))
    packet[members:] = jnp.concatenate(rows, axis=0)
    above = jnp.sum(innovation * innovation)
    below = jnp.sum(spread + error[...])
    lane = lax.broadcasted_iota(jnp.int32, sums.shape, 1)
    sums[...] = jnp.where(lane == 0, above, jnp.where(lane == 1, below, 0.0))


def stats(me, gathered, values, error, tiles, regions):
    peers = len(gathered)
    own, obs = gathered[0].shape
    return pl.pallas_call(
        stats_body,
        in_specs=[scalars()] + [whole()] * (3 + peers),
        out_specs=[whole(), whole()],
        out_shape=[shape_of((peers * own + 16, obs)), shape_of((regions, 128), F32)],
        scratch_shapes=[pltpu.VMEM((peers, 8, obs), F32)],
        compiler_params=params(),
        name="stats",
    )(me, values, error, tiles, *gathered)


def scalar_rows(rows):
    rows = rows.astype(F32)
    innovation = rows[0:1] + rows[1:2] + rows[2:3]
    error = rows[3:4] + rows[4:5] + rows[5:6]
    spread = rows[6:7] + rows[7:8] + rows[8:9]
    return innovation, error, spread, rows[9:10] * 32.0 + rows[10:11]


def gains(state, anom_t, taper, means, anomalies, gain):
    own = state[0].shape[0]
    parts = [part.astype(F32) for part in state]
    mean = sum(jnp.sum(part, axis=0, keepdims=True) for part in parts) / (own * len(parts))
    means[...] = jnp.broadcast_to(mean, means.shape)
    for s, part in enumerate(parts):
        anomalies[s * own : (s + 1) * own] = (part - mean).astype(BF16)
    at = 0
    for some_t, tapers in zip(anom_t, taper):
        covariance = jnp.dot(some_t[...], anomalies[...], preferred_element_type=F32)
        gain[at : at + tapers.shape[0]] = (covariance * tapers[...]).astype(BF16)
        at += tapers.shape[0]


def posterior(gain, means, anomalies, perturbed, root, blocks, at):
    own = blocks[0].shape[1]
    increment = jnp.dot(perturbed[...], gain[...], preferred_element_type=F32)
    result = means[0:1] + root * anomalies[...].astype(F32) + increment
    for s, block in enumerate(blocks):
        block[at] = result[s * own : (s + 1) * own].astype(BF16)


def tapers(scales, offset, side, width, members, tile_count):
    tile = (offset[0] + lax.broadcasted_iota(jnp.int32, (1, width), 1)).astype(F32)
    place = scalar_rows(scales)[3] + (offset[side] * tile_count).astype(F32)
    column = jnp.broadcast_to(place, (8, place.shape[1])).T[:, 0:1]
    near = jnp.maximum(0.0, 1.0 - jnp.abs(tile - column) / RADIUS)
    return near * near / (members - 1)


def prepare_body(offset, *refs, tile_count):
    *far_packets, anom_t, taper, packets, arrived = refs
    members = anom_t.shape[1]
    obs = packets.shape[2]
    loads = [
        pltpu.make_async_copy(packet, packets.at[n], arrived.at[n])
        for n, packet in enumerate(far_packets)
    ]
    for load in loads:
        load.start()
    for n, load in enumerate(loads):
        load.wait()
        rows = slice(n * obs, (n + 1) * obs)
        anom_t[rows] = packets[n, :members].T
        taper[rows] = tapers(packets[n, members:], offset, 1 + n, taper.shape[1], members, tile_count)


def prepare(offset, packets, width, tile_count):
    rows, obs = packets[0].shape
    members = rows - 16
    count = len(packets)
    return pl.pallas_call(
        functools.partial(prepare_body, tile_count=tile_count),
        in_specs=[scalars()] + [anywhere()] * count,
        out_specs=[whole()] * 2,
        out_shape=[shape_of((count * obs, members)), shape_of((count * obs, width), F32)],
        scratch_shapes=[
            pltpu.VMEM((count, rows, obs), BF16),
            pltpu.SemaphoreType.DMA((count,)),
        ],
        compiler_params=params(),
        name="prepare",
    )(offset, *map(in_hbm, packets))


def start_body(offset, *refs, peers, tile_count):
    far_states, far_packets = refs[:peers], refs[peers : peers + 3]
    anom_0, taper_0, anom_2, taper_2, means, anomalies, gain, packets, rest = refs[peers + 3 : peers + 12]
    states, arrived, near, passed = refs[peers + 12 :]
    members, width = anomalies.shape[1:]
    count = gain.shape[0]
    loads = [
        pltpu.make_async_copy(far_states[s].at[:count], states.at[s], arrived.at[s])
        for s in range(peers)
    ]
    late = [
        pltpu.make_async_copy(far_packets[n], packets.at[n], near.at[n]) for n in range(3)
    ]
    onward = [
        pltpu.make_async_copy(far_states[s].at[count:], rest.at[s], passed.at[s])
        for s in range(peers)
    ]
    for load in [late[2], *loads, late[0], late[1], *onward]:
        load.start()
    late[2].wait()
    anom_2[...] = packets[2, :members].T
    taper_2[...] = tapers(packets[2, members:], offset, 3, width, members, tile_count)
    for load in loads:
        load.wait()
    for l in range(count):
        state = [states[s, l] for s in range(peers)]
        gains(
            state, (anom_0, anom_2), (taper_0, taper_2), means.at[l], anomalies.at[l], gain.at[l]
        )
    for load in [late[0], late[1], *onward]:
        load.wait()


def start_gains(offset, states, packets, anom_0, taper_0, count, tile_count):
    var_count, own, width = states[0].shape
    peers = len(states)
    members = own * peers
    rows, obs = packets[0].shape
    return pl.pallas_call(
        functools.partial(start_body, peers=peers, tile_count=tile_count),
        in_specs=[scalars()] + [anywhere()] * (peers + 3) + [whole()] * 2,
        out_specs=[whole()] * 7,
        out_shape=[
            shape_of((obs, members)),
            shape_of((obs, width), F32),
            shape_of((count, 8, width), F32),
            shape_of((count, members, width)),
            shape_of((count, 3 * obs, width)),
            shape_of((3, rows, obs)),
            shape_of((peers, var_count - count, own, width)),
        ],
        scratch_shapes=[
            pltpu.VMEM((peers, count, own, width), BF16),
            pltpu.SemaphoreType.DMA((peers,)),
            pltpu.SemaphoreType.DMA((3,)),
            pltpu.SemaphoreType.DMA((peers,)),
        ],
        compiler_params=params(8),
        name="start",
    )(
        offset,
        in_hbm(states[0]),
        *states[1:],
        *map(in_hbm, packets),
        *in_vmem((anom_0, taper_0)),
    )


def first_body(means, anomalies, gain, packets, sums, *refs):
    noises, (*blocks, perturbed, root_out, inflation_out) = refs[:3], refs[3:]
    members = anomalies.shape[1]
    obs = packets.shape[2]
    folded = jnp.sum(sums[...], axis=0, keepdims=True)
    inflation = folded[:, 0:1] / folded[:, 1:2]
    inflation_out[0] = jnp.sum(inflation)
    root = jnp.sqrt(inflation)
    root_out[...] = jnp.broadcast_to(root, root_out.shape)
    for n in range(3):
        innovation, error, spread, _ = scalar_rows(packets[n, members:])
        bottom = jnp.where(error > 0.0, inflation * spread + error, 1.0)
        factor = jnp.where(error > 0.0, inflation / bottom, 0.0)
        dev = packets[n, :members].astype(F32)
        perturbed[:, n * obs : (n + 1) * obs] = (
            factor * (innovation + noises[n][...].astype(F32) - root * dev)
        ).astype(BF16)
    for l in range(gain.shape[0]):
        posterior(gain.at[l], means.at[l], anomalies.at[l], perturbed, root, blocks, l)


def working(count, members, obs, width):
    return [
        pltpu.VMEM((count, 8, width), F32),
        pltpu.VMEM((count, members, width), BF16),
        pltpu.VMEM((count, obs, width), BF16),
    ]


def first_updates(means, anomalies, gain, packets, sums, noises, peers):
    count, members, width = anomalies.shape
    obs = packets.shape[2]
    out = pl.pallas_call(
        first_body,
        in_specs=[whole()] * 8,
        out_specs=[whole()] * (peers + 2) + [scalars()],
        out_shape=[shape_of((count, members // peers, width))] * peers
        + [
            shape_of((members, 3 * obs)),
            shape_of((8, 128), F32),
            jax.ShapeDtypeStruct((1,), F32),
        ],
        compiler_params=params(4),
        name="first",
    )(*in_vmem((means, anomalies, gain, packets, sums, *noises)))
    return out[:peers], *out[peers:]


def second_body(states, perturbed, root, *refs):
    shared, (*blocks, means, anomalies, gain) = refs[:4], refs[4:]
    peers = len(blocks)
    count = blocks[0].shape[0]
    for l in range(count):
        state = [states[s, l] for s in range(peers)]
        gains(state, shared[:2], shared[2:], means.at[l], anomalies.at[l], gain.at[l])
    for l in range(count):
        posterior(gain.at[l], means.at[l], anomalies.at[l], perturbed, root[0:1, 0:1], blocks, l)


def second_updates(states, perturbed, root, shared):
    peers, count, own, width = states.shape
    return pl.pallas_call(
        second_body,
        in_specs=[whole()] * 7,
        out_specs=[whole()] * peers,
        out_shape=[shape_of((count, own, width))] * peers,
        scratch_shapes=working(count, peers * own, perturbed.shape[1], width),
        compiler_params=params(),
        name="second",
    )(*in_vmem((states, perturbed, root, *shared)))


def place_body(me, *refs, first, peers):
    blocks, out, done = refs[:peers], refs[-2], refs[-1]
    count, _, width = blocks[0].shape
    copies = [
        pltpu.make_async_copy(
            blocks[s],
            out.at[first : first + count, :, pl.ds(tile_block(me[0], s, width), width)],
            done.at[s],
        )
        for s in range(peers)
    ]
    for copy in copies:
        copy.start()
    for copy in copies:
        copy.wait()


def place(me, blocks, first, var_count, before=None):
    peers = len(blocks)
    _, own, width = blocks[0].shape
    more = [] if before is None else [before]
    return pl.pallas_call(
        functools.partial(place_body, first=first, peers=peers),
        in_specs=[scalars()] + [anywhere()] * (peers + len(more)),
        out_specs=anywhere(),
        out_shape=pltpu.HBM((var_count, own, peers * width), BF16),
        scratch_shapes=[pltpu.SemaphoreType.DMA((peers,))],
        input_output_aliases={1 + peers: 0} if more else {},
        compiler_params=params(),
    )(me, *in_vmem(blocks), *more)


def swapped(value, axis, distance):
    pairs = [(i, i ^ distance) for i in range(lax.axis_size(axis))]
    return lax.ppermute(value, axis, pairs)


def exchanged(blocks, axis):
    return lax.all_to_all(blocks, axis, split_axis=0, concat_axis=0, tiled=True)


def traded(blocks, order):
    out = list(blocks)
    for s in order:
        out[s] = swapped(blocks[s], "member", s)
    return out


def shards(ensemble, obs_weights, obs_tiles, obs_values, obs_error, obs_noise):
    peers = lax.axis_size("member")
    regions = lax.axis_size("region")
    var_count, _, tile_count = ensemble.shape
    width = tile_count // peers
    me = lax.axis_index("member").astype(jnp.int32)[None]
    region = lax.axis_index("region").astype(jnp.int32)
    tiles, values, error = (a[None, :] for a in (obs_tiles, obs_values, obs_error))
    *blocks, partial = pack(me, ensemble, obs_weights, tiles, peers)
    other = swapped(partial, "depth", 1)
    noises = traded([scale(obs_noise, error)] * peers, (1, 3, 2))
    predicted = traded([join(partial, other)] * peers, (1, 3, 2))
    pairs = [(i, i + 1) for i in range(1, regions - 1, 2)]
    pairs += [(j, i) for i, j in pairs]
    packet, sums = stats(me, predicted, values, error, tiles, regions)
    near = swapped(packet, "region", 1)
    far = lax.ppermute(packet, "region", pairs)
    states = traded(blocks, (1, 3, 2))
    all_sums = exchanged(sums, "region")
    noise = join_noise(noises)
    near_noise = swapped(noise, "region", 1)
    far_noise = lax.ppermute(noise, "region", pairs)
    side = 1 - 2 * (region % 2)
    offset = jnp.stack([me[0] * width, jnp.zeros_like(side), side, -side])
    anom_0, taper_0 = prepare(offset, (packet, near), width, tile_count)
    half = (var_count + 1) // 2
    anom_2, taper_2, means, anomalies, gain, packets, rest = start_gains(
        offset, states, (packet, near, far), anom_0, taper_0, half, tile_count
    )
    ready, perturbed, root, inflation = first_updates(
        means, anomalies, gain, packets, all_sums, (noise, near_noise, far_noise), peers
    )
    shared = (anom_0, anom_2, taper_0, taper_2)
    early = traded(ready, (1, 3, 2))
    ready = second_updates(rest, perturbed, root, shared)
    late = traded(ready, (1, 3, 2))
    output = place(me, early, 0, var_count)
    output = place(me, late, half, var_count, output)
    return (output, inflation.reshape(()))


def solution(mesh):
    return jax.shard_map(
        shards,
        mesh=mesh,
        in_specs=(
            P("depth", "member", "region"),
            P("depth"),
            P("region"),
            P("region"),
            P("region"),
            P("member", "region"),
        ),
        out_specs=(P("depth", "member", "region"), P()),
        check_vma=False,
    )
```

```python
import functools

import jax
import jax.numpy as jnp
from jax import lax
from jax.experimental import pallas as pl
from jax.experimental.pallas import tpu as pltpu
from jax.sharding import PartitionSpec as P


RADIUS = 1024
F32 = jnp.float32
BF16 = jnp.bfloat16


def params(megabytes=12):
    return pltpu.CompilerParams(vmem_limit_bytes=megabytes * 2**20)


def whole():
    return pl.BlockSpec(memory_space=pltpu.VMEM)


def scalars():
    return pl.BlockSpec(memory_space=pltpu.SMEM)


def anywhere():
    return pl.BlockSpec(memory_space=pl.ANY)


def shape_of(shape, dtype=BF16):
    return pltpu.VMEM(shape, dtype)


def in_vmem(values):
    return [pltpu.with_memory_space_constraint(v, pltpu.VMEM) for v in values]


def in_hbm(value):
    return pltpu.with_memory_space_constraint(value, pltpu.HBM)


def split_rows(value):
    first = value.astype(BF16)
    rest = value - first.astype(F32)
    second = rest.astype(BF16)
    third = (rest - second.astype(F32)).astype(BF16)
    return [first, second, third]


def tile_block(me, s, width):
    return pl.multiple_of(jnp.bitwise_xor(me, s) * width, width)


def pack_body(me, far_weights, ensemble, far_tiles, *rest):
    *blocks, predicted, weights, tiles, chosen, halves, buffer, arrived, left = rest
    peers, var_count, _, width = buffer.shape
    starts = [tile_block(me[0], s, width) for s in range(peers)]
    loads = [
        pltpu.make_async_copy(
            ensemble.at[:, :, pl.ds(starts[s], width)], buffer.at[s], arrived.at[s]
        )
        for s in range(peers)
    ]
    stores = [pltpu.make_async_copy(buffer.at[s], blocks[s], left.at[s]) for s in range(peers)]
    light = [
        pltpu.make_async_copy(far_weights, weights, arrived.at[peers]),
        pltpu.make_async_copy(far_tiles, tiles, arrived.at[peers + 1]),
    ]
    for load in light + loads:
        load.start()
    for load in light:
        load.wait()
    rows = lax.broadcasted_iota(jnp.int32, (width, tiles.shape[1]), 0)
    for s in range(peers):
        chosen[s * width : (s + 1) * width] = jnp.where(
            tiles[...] - starts[s] == rows, 1.0, 0.0
        ).astype(BF16)
    for s in range(peers):
        loads[s].wait()
        stores[s].start()
        mixed = weights[0] * buffer[s, 0].astype(F32)
        for l in range(1, var_count):
            mixed = mixed + weights[l] * buffer[s, l].astype(F32)
        high = mixed.astype(BF16)
        columns = slice(s * width, (s + 1) * width)
        halves[: mixed.shape[0], columns] = high
        halves[mixed.shape[0] :, columns] = (mixed - high.astype(F32)).astype(BF16)
    picked = jnp.dot(halves[...], chosen[...], preferred_element_type=F32)
    own = predicted.shape[0]
    predicted[...] = (picked[:own] + picked[own:]).astype(BF16)
    for store in stores:
        store.wait()


def pack(me, ensemble, weights, tiles, peers):
    var_count, own, tile_count = ensemble.shape
    width = tile_count // peers
    obs = tiles.shape[1]
    return pl.pallas_call(
        pack_body,
        in_specs=[scalars()] + [anywhere()] * 3,
        out_specs=[anywhere()] * peers + [whole()],
        out_shape=[pltpu.HBM((var_count, own, width), BF16)] * peers + [shape_of((own, obs))],
        scratch_shapes=[
            pltpu.SMEM((var_count,), F32),
            pltpu.VMEM((1, obs), jnp.int32),
            pltpu.VMEM((tile_count, obs), BF16),
            pltpu.VMEM((2 * own, tile_count), BF16),
            pltpu.VMEM((peers, var_count, own, width), BF16),
            pltpu.SemaphoreType.DMA((peers + 2,)),
            pltpu.SemaphoreType.DMA((peers,)),
        ],
        compiler_params=params(),
        name="pack",
    )(me, in_hbm(weights), in_hbm(ensemble), in_hbm(tiles))


def scale_body(noise, error, out):
    out[...] = (jnp.sqrt(error[...]) * noise[...]).astype(BF16)


def scale(noise, error):
    return pl.pallas_call(
        scale_body,
        in_specs=[whole()] * 2,
        out_specs=whole(),
        out_shape=shape_of(noise.shape),
        compiler_params=params(),
        name="scale",
    )(noise, error)


def join_noise_body(*refs):
    *parts, out = refs
    own = parts[0].shape[0]
    for s, part in enumerate(parts):
        out[s * own : (s + 1) * own] = part[...]


def join_noise(parts):
    own, obs = parts[0].shape
    return pl.pallas_call(
        join_noise_body,
        in_specs=[whole()] * len(parts),
        out_specs=whole(),
        out_shape=shape_of((len(parts) * own, obs)),
        compiler_params=params(),
        name="joinnoise",
    )(*parts)


def join_body(mine, other, out):
    out[...] = (mine[...].astype(F32) + other[...].astype(F32)).astype(BF16)


def join(mine, other):
    return pl.pallas_call(
        join_body,
        in_specs=[whole()] * 2,
        out_specs=whole(),
        out_shape=shape_of(mine.shape),
        compiler_params=params(),
        name="join",
    )(mine, other)


def stats_body(me, values, error, tiles, *refs):
    *gathered, packet, sums, ordered = refs
    peers = len(gathered)
    own, obs = gathered[0].shape
    members = peers * own
    for s in range(peers):
        part = jnp.sum(gathered[s][...].astype(F32), axis=0, keepdims=True)
        ordered[jnp.bitwise_xor(me[0], s)] = jnp.broadcast_to(part, ordered.shape[1:])
    mean = (ordered[0] + ordered[1] + ordered[2] + ordered[3])[0:1] / members
    for s in range(peers):
        dev = gathered[s][...].astype(F32) - mean
        packet[s * own : (s + 1) * own] = dev.astype(BF16)
        part = jnp.sum(dev * dev, axis=0, keepdims=True)
        ordered[jnp.bitwise_xor(me[0], s)] = jnp.broadcast_to(part, ordered.shape[1:])
    spread = (ordered[0] + ordered[1] + ordered[2] + ordered[3])[0:1] / (members - 1)
    innovation = values[...] - mean
    place = tiles[...]
    rows = split_rows(innovation) + split_rows(error[...]) + split_rows(spread)
    rows += [(place // 32).astype(F32).astype(BF16), (place % 32).astype(F32).astype(BF16)]
    rows += [jnp.zeros((1, obs), BF16)] * (16 - len(rows))
    packet[members:] = jnp.concatenate(rows, axis=0)
    above = jnp.sum(innovation * innovation)
    below = jnp.sum(spread + error[...])
    lane = lax.broadcasted_iota(jnp.int32, sums.shape, 1)
    sums[...] = jnp.where(lane == 0, above, jnp.where(lane == 1, below, 0.0))


def stats(me, gathered, values, error, tiles, regions):
    peers = len(gathered)
    own, obs = gathered[0].shape
    return pl.pallas_call(
        stats_body,
        in_specs=[scalars()] + [whole()] * (3 + peers),
        out_specs=[whole(), whole()],
        out_shape=[shape_of((peers * own + 16, obs)), shape_of((regions, 128), F32)],
        scratch_shapes=[pltpu.VMEM((peers, 8, obs), F32)],
        compiler_params=params(),
        name="stats",
    )(me, values, error, tiles, *gathered)


def scalar_rows(rows):
    rows = rows.astype(F32)
    innovation = rows[0:1] + rows[1:2] + rows[2:3]
    error = rows[3:4] + rows[4:5] + rows[5:6]
    spread = rows[6:7] + rows[7:8] + rows[8:9]
    return innovation, error, spread, rows[9:10] * 32.0 + rows[10:11]


def gains(state, anom_t, taper, means, anomalies, gain):
    own = state[0].shape[0]
    parts = [part.astype(F32) for part in state]
    mean = sum(jnp.sum(part, axis=0, keepdims=True) for part in parts) / (own * len(parts))
    means[...] = jnp.broadcast_to(mean, means.shape)
    for s, part in enumerate(parts):
        anomalies[s * own : (s + 1) * own] = (part - mean).astype(BF16)
    at = 0
    for some_t, tapers in zip(anom_t, taper):
        covariance = jnp.dot(some_t[...], anomalies[...], preferred_element_type=F32)
        gain[at : at + tapers.shape[0]] = (covariance * tapers[...]).astype(BF16)
        at += tapers.shape[0]


def posterior(gain, means, anomalies, perturbed, root, blocks, at):
    own = blocks[0].shape[1]
    increment = jnp.dot(perturbed[...], gain[...], preferred_element_type=F32)
    result = means[0:1] + root * anomalies[...].astype(F32) + increment
    for s, block in enumerate(blocks):
        block[at] = result[s * own : (s + 1) * own].astype(BF16)


def tapers(scales, offset, side, width, members, tile_count):
    tile = (offset[0] + lax.broadcasted_iota(jnp.int32, (1, width), 1)).astype(F32)
    place = scalar_rows(scales)[3] + (offset[side] * tile_count).astype(F32)
    column = jnp.broadcast_to(place, (8, place.shape[1])).T[:, 0:1]
    near = jnp.maximum(0.0, 1.0 - jnp.abs(tile - column) / RADIUS)
    return near * near / (members - 1)


def prepare_body(offset, *refs, tile_count):
    *packets, anom_t, taper = refs
    members = anom_t.shape[1]
    obs = packets[0].shape[1]
    for n, packet in enumerate(packets):
        rows = slice(n * obs, (n + 1) * obs)
        anom_t[rows] = packet[:members].T
        taper[rows] = tapers(packet[members:], offset, 1 + n, taper.shape[1], members, tile_count)


def prepare(offset, packets, width, tile_count):
    rows, obs = packets[0].shape
    members = rows - 16
    count = len(packets)
    return pl.pallas_call(
        functools.partial(prepare_body, tile_count=tile_count),
        in_specs=[scalars()] + [whole()] * count,
        out_specs=[whole()] * 2,
        out_shape=[shape_of((count * obs, members)), shape_of((count * obs, width), F32)],
        compiler_params=params(4),
        name="prepare",
    )(offset, *in_vmem(packets))


def start_body(offset, *refs, peers, tile_count):
    far_states, far_packets = refs[:peers], refs[peers : peers + 3]
    anom_0, taper_0, anom_2, taper_2, means, anomalies, gain, packets, rest = refs[peers + 3 : peers + 12]
    states, arrived, near, passed = refs[peers + 12 :]
    members, width = anomalies.shape[1:]
    count = gain.shape[0]
    loads = [
        pltpu.make_async_copy(far_states[s].at[:count], states.at[s], arrived.at[s])
        for s in range(peers)
    ]
    late = [
        pltpu.make_async_copy(far_packets[n], packets.at[n], near.at[n]) for n in range(3)
    ]
    onward = [
        pltpu.make_async_copy(far_states[s].at[count:], rest.at[s], passed.at[s])
        for s in range(peers)
    ]
    for load in [late[2], *loads, late[0], late[1], *onward]:
        load.start()
    late[2].wait()
    anom_2[...] = packets[2, :members].T
    taper_2[...] = tapers(packets[2, members:], offset, 3, width, members, tile_count)
    for load in loads:
        load.wait()
    for l in range(count):
        state = [states[s, l] for s in range(peers)]
        gains(
            state, (anom_0, anom_2), (taper_0, taper_2), means.at[l], anomalies.at[l], gain.at[l]
        )
    for load in [late[0], late[1], *onward]:
        load.wait()


def start_gains(offset, states, packets, anom_0, taper_0, count, tile_count):
    var_count, own, width = states[0].shape
    peers = len(states)
    members = own * peers
    rows, obs = packets[0].shape
    return pl.pallas_call(
        functools.partial(start_body, peers=peers, tile_count=tile_count),
        in_specs=[scalars()] + [anywhere()] * (peers + 3) + [whole()] * 2,
        out_specs=[whole()] * 7,
        out_shape=[
            shape_of((obs, members)),
            shape_of((obs, width), F32),
            shape_of((count, 8, width), F32),
            shape_of((count, members, width)),
            shape_of((count, 3 * obs, width)),
            shape_of((3, rows, obs)),
            shape_of((peers, var_count - count, own, width)),
        ],
        scratch_shapes=[
            pltpu.VMEM((peers, count, own, width), BF16),
            pltpu.SemaphoreType.DMA((peers,)),
            pltpu.SemaphoreType.DMA((3,)),
            pltpu.SemaphoreType.DMA((peers,)),
        ],
        compiler_params=params(8),
        name="start",
    )(
        offset,
        in_hbm(states[0]),
        *states[1:],
        *map(in_hbm, packets),
        *in_vmem((anom_0, taper_0)),
    )


def first_body(means, anomalies, gain, packets, sums, noise_0, noise_1, far_noise, *refs):
    *blocks, perturbed, root_out, inflation_out, noise_2, arrived = refs
    members = anomalies.shape[1]
    obs = packets.shape[2]
    load = pltpu.make_async_copy(far_noise, noise_2, arrived)
    load.start()
    folded = jnp.sum(sums[...], axis=0, keepdims=True)
    inflation = folded[:, 0:1] / folded[:, 1:2]
    inflation_out[0] = jnp.sum(inflation)
    root = jnp.sqrt(inflation)
    root_out[...] = jnp.broadcast_to(root, root_out.shape)
    for n, noise in enumerate((noise_0, noise_1, noise_2)):
        if n == 2:
            load.wait()
        innovation, error, spread, _ = scalar_rows(packets[n, members:])
        bottom = jnp.where(error > 0.0, inflation * spread + error, 1.0)
        factor = jnp.where(error > 0.0, inflation / bottom, 0.0)
        dev = packets[n, :members].astype(F32)
        perturbed[:, n * obs : (n + 1) * obs] = (
            factor * (innovation + noise[...].astype(F32) - root * dev)
        ).astype(BF16)
    for l in range(gain.shape[0]):
        posterior(gain.at[l], means.at[l], anomalies.at[l], perturbed, root, blocks, l)


def working(count, members, obs, width):
    return [
        pltpu.VMEM((count, 8, width), F32),
        pltpu.VMEM((count, members, width), BF16),
        pltpu.VMEM((count, obs, width), BF16),
    ]


def first_updates(means, anomalies, gain, packets, sums, noises, peers):
    count, members, width = anomalies.shape
    obs = packets.shape[2]
    out = pl.pallas_call(
        first_body,
        in_specs=[whole()] * 7 + [anywhere()],
        out_specs=[whole()] * (peers + 2) + [scalars()],
        out_shape=[shape_of((count, members // peers, width))] * peers
        + [
            shape_of((members, 3 * obs)),
            shape_of((8, 128), F32),
            jax.ShapeDtypeStruct((1,), F32),
        ],
        scratch_shapes=[pltpu.VMEM(noises[2].shape, BF16), pltpu.SemaphoreType.DMA],
        compiler_params=params(4),
        name="first",
    )(*in_vmem((means, anomalies, gain, packets, sums, *noises[:2])), noises[2])
    return out[:peers], *out[peers:]


def second_body(states, perturbed, root, *refs):
    shared, (*blocks, means, anomalies, gain) = refs[:4], refs[4:]
    peers = len(blocks)
    count = blocks[0].shape[0]
    for l in range(count):
        state = [states[s, l] for s in range(peers)]
        gains(state, shared[:2], shared[2:], means.at[l], anomalies.at[l], gain.at[l])
    for l in range(count):
        posterior(gain.at[l], means.at[l], anomalies.at[l], perturbed, root[0:1, 0:1], blocks, l)


def second_updates(states, perturbed, root, shared):
    peers, count, own, width = states.shape
    return pl.pallas_call(
        second_body,
        in_specs=[whole()] * 7,
        out_specs=[whole()] * peers,
        out_shape=[shape_of((count, own, width))] * peers,
        scratch_shapes=working(count, peers * own, perturbed.shape[1], width),
        compiler_params=params(),
        name="second",
    )(*in_vmem((states, perturbed, root, *shared)))


def place_body(me, *refs, first, peers):
    blocks, out, done = refs[:peers], refs[-2], refs[-1]
    count, _, width = blocks[0].shape
    copies = [
        pltpu.make_async_copy(
            blocks[s],
            out.at[first : first + count, :, pl.ds(tile_block(me[0], s, width), width)],
            done.at[s],
        )
        for s in range(peers)
    ]
    for copy in copies:
        copy.start()
    for copy in copies:
        copy.wait()


def place(me, blocks, first, var_count, before=None):
    peers = len(blocks)
    _, own, width = blocks[0].shape
    more = [] if before is None else [before]
    return pl.pallas_call(
        functools.partial(place_body, first=first, peers=peers),
        in_specs=[scalars()] + [anywhere()] * (peers + len(more)),
        out_specs=anywhere(),
        out_shape=pltpu.HBM((var_count, own, peers * width), BF16),
        scratch_shapes=[pltpu.SemaphoreType.DMA((peers,))],
        input_output_aliases={1 + peers: 0} if more else {},
        compiler_params=params(),
    )(me, *in_vmem(blocks), *more)


def swapped(value, axis, distance):
    pairs = [(i, i ^ distance) for i in range(lax.axis_size(axis))]
    return lax.ppermute(value, axis, pairs)


def exchanged(blocks, axis):
    return lax.all_to_all(blocks, axis, split_axis=0, concat_axis=0, tiled=True)


def traded(blocks, order):
    out = list(blocks)
    for s in order:
        out[s] = swapped(blocks[s], "member", s)
    return out


def shards(ensemble, obs_weights, obs_tiles, obs_values, obs_error, obs_noise):
    peers = lax.axis_size("member")
    regions = lax.axis_size("region")
    var_count, _, tile_count = ensemble.shape
    width = tile_count // peers
    me = lax.axis_index("member").astype(jnp.int32)[None]
    region = lax.axis_index("region").astype(jnp.int32)
    tiles, values, error = (a[None, :] for a in (obs_tiles, obs_values, obs_error))
    *blocks, partial = pack(me, ensemble, obs_weights, tiles, peers)
    other = swapped(partial, "depth", 1)
    noises = traded([scale(obs_noise, error)] * peers, (1, 3, 2))
    predicted = traded([join(partial, other)] * peers, (1, 3, 2))
    pairs = [(i, i + 1) for i in range(1, regions - 1, 2)]
    pairs += [(j, i) for i, j in pairs]
    packet, sums = stats(me, predicted, values, error, tiles, regions)
    near = swapped(packet, "region", 1)
    far = lax.ppermute(packet, "region", pairs)
    states = traded(blocks, (1, 3, 2))
    all_sums = exchanged(sums, "region")
    noise = join_noise(noises)
    near_noise = swapped(noise, "region", 1)
    far_noise = lax.ppermute(noise, "region", pairs)
    side = 1 - 2 * (region % 2)
    offset = jnp.stack([me[0] * width, jnp.zeros_like(side), side, -side])
    anom_0, taper_0 = prepare(offset, (packet, near), width, tile_count)
    half = (var_count + 1) // 2
    anom_2, taper_2, means, anomalies, gain, packets, rest = start_gains(
        offset, states, (packet, near, far), anom_0, taper_0, half, tile_count
    )
    ready, perturbed, root, inflation = first_updates(
        means, anomalies, gain, packets, all_sums, (noise, near_noise, far_noise), peers
    )
    shared = (anom_0, anom_2, taper_0, taper_2)
    early = traded(ready, (1, 3, 2))
    ready = second_updates(rest, perturbed, root, shared)
    late = traded(ready, (1, 3, 2))
    output = place(me, early, 0, var_count)
    output = place(me, late, half, var_count, output)
    return (output, inflation.reshape(()))


def solution(mesh):
    return jax.shard_map(
        shards,
        mesh=mesh,
        in_specs=(
            P("depth", "member", "region"),
            P("depth"),
            P("region"),
            P("region"),
            P("region"),
            P("member", "region"),
        ),
        out_specs=(P("depth", "member", "region"), P()),
        check_vma=False,
    )
```

```python
import functools

import jax
import jax.numpy as jnp
from jax import lax
from jax.experimental import pallas as pl
from jax.experimental.pallas import tpu as pltpu
from jax.sharding import PartitionSpec as P


RADIUS = 1024
F32 = jnp.float32
BF16 = jnp.bfloat16


def params(megabytes=12):
    return pltpu.CompilerParams(vmem_limit_bytes=megabytes * 2**20)


def whole():
    return pl.BlockSpec(memory_space=pltpu.VMEM)


def scalars():
    return pl.BlockSpec(memory_space=pltpu.SMEM)


def anywhere():
    return pl.BlockSpec(memory_space=pl.ANY)


def shape_of(shape, dtype=BF16):
    return pltpu.VMEM(shape, dtype)


def in_vmem(values):
    return [pltpu.with_memory_space_constraint(v, pltpu.VMEM) for v in values]


def in_hbm(value):
    return pltpu.with_memory_space_constraint(value, pltpu.HBM)


def split_rows(value):
    first = value.astype(BF16)
    rest = value - first.astype(F32)
    second = rest.astype(BF16)
    third = (rest - second.astype(F32)).astype(BF16)
    return [first, second, third]


def tile_block(me, s, width):
    return pl.multiple_of(jnp.bitwise_xor(me, s) * width, width)


def pack_body(me, far_weights, ensemble, far_tiles, *rest):
    *blocks, predicted, weights, tiles, chosen, halves, buffer, arrived, left = rest
    peers, var_count, _, width = buffer.shape
    starts = [tile_block(me[0], s, width) for s in range(peers)]
    loads = [
        pltpu.make_async_copy(
            ensemble.at[:, :, pl.ds(starts[s], width)], buffer.at[s], arrived.at[s]
        )
        for s in range(peers)
    ]
    stores = [pltpu.make_async_copy(buffer.at[s], blocks[s], left.at[s]) for s in range(peers)]
    light = [
        pltpu.make_async_copy(far_weights, weights, arrived.at[peers]),
        pltpu.make_async_copy(far_tiles, tiles, arrived.at[peers + 1]),
    ]
    for load in light + loads:
        load.start()
    for load in light:
        load.wait()
    rows = lax.broadcasted_iota(jnp.int32, (width, tiles.shape[1]), 0)
    for s in range(peers):
        chosen[s * width : (s + 1) * width] = jnp.where(
            tiles[...] - starts[s] == rows, 1.0, 0.0
        ).astype(BF16)
    for s in range(peers):
        loads[s].wait()
        stores[s].start()
        mixed = weights[0] * buffer[s, 0].astype(F32)
        for l in range(1, var_count):
            mixed = mixed + weights[l] * buffer[s, l].astype(F32)
        high = mixed.astype(BF16)
        columns = slice(s * width, (s + 1) * width)
        halves[: mixed.shape[0], columns] = high
        halves[mixed.shape[0] :, columns] = (mixed - high.astype(F32)).astype(BF16)
    picked = jnp.dot(halves[...], chosen[...], preferred_element_type=F32)
    own = predicted.shape[0]
    predicted[...] = (picked[:own] + picked[own:]).astype(BF16)
    for store in stores:
        store.wait()


def pack(me, ensemble, weights, tiles, peers):
    var_count, own, tile_count = ensemble.shape
    width = tile_count // peers
    obs = tiles.shape[1]
    return pl.pallas_call(
        pack_body,
        in_specs=[scalars()] + [anywhere()] * 3,
        out_specs=[anywhere()] * peers + [whole()],
        out_shape=[pltpu.HBM((var_count, own, width), BF16)] * peers + [shape_of((own, obs))],
        scratch_shapes=[
            pltpu.SMEM((var_count,), F32),
            pltpu.VMEM((1, obs), jnp.int32),
            pltpu.VMEM((tile_count, obs), BF16),
            pltpu.VMEM((2 * own, tile_count), BF16),
            pltpu.VMEM((peers, var_count, own, width), BF16),
            pltpu.SemaphoreType.DMA((peers + 2,)),
            pltpu.SemaphoreType.DMA((peers,)),
        ],
        compiler_params=params(),
        name="pack",
    )(me, in_hbm(weights), in_hbm(ensemble), in_hbm(tiles))


def scale_body(noise, error, out):
    out[...] = (jnp.sqrt(error[...]) * noise[...]).astype(BF16)


def scale(noise, error):
    return pl.pallas_call(
        scale_body,
        in_specs=[whole()] * 2,
        out_specs=whole(),
        out_shape=shape_of(noise.shape),
        compiler_params=params(),
        name="scale",
    )(noise, error)


def join_noise_body(*refs):
    *parts, out = refs
    own = parts[0].shape[0]
    for s, part in enumerate(parts):
        out[s * own : (s + 1) * own] = part[...]


def join_noise(parts):
    own, obs = parts[0].shape
    return pl.pallas_call(
        join_noise_body,
        in_specs=[whole()] * len(parts),
        out_specs=whole(),
        out_shape=shape_of((len(parts) * own, obs)),
        compiler_params=params(),
        name="joinnoise",
    )(*parts)


def join_body(mine, other, out):
    out[...] = (mine[...].astype(F32) + other[...].astype(F32)).astype(BF16)


def join(mine, other):
    return pl.pallas_call(
        join_body,
        in_specs=[whole()] * 2,
        out_specs=whole(),
        out_shape=shape_of(mine.shape),
        compiler_params=params(),
        name="join",
    )(mine, other)


def stats_body(me, values, error, tiles, *refs):
    *gathered, packet, sums, ordered = refs
    peers = len(gathered)
    own, obs = gathered[0].shape
    members = peers * own
    for s in range(peers):
        part = jnp.sum(gathered[s][...].astype(F32), axis=0, keepdims=True)
        ordered[jnp.bitwise_xor(me[0], s)] = jnp.broadcast_to(part, ordered.shape[1:])
    mean = (ordered[0] + ordered[1] + ordered[2] + ordered[3])[0:1] / members
    for s in range(peers):
        dev = gathered[s][...].astype(F32) - mean
        packet[s * own : (s + 1) * own] = dev.astype(BF16)
        part = jnp.sum(dev * dev, axis=0, keepdims=True)
        ordered[jnp.bitwise_xor(me[0], s)] = jnp.broadcast_to(part, ordered.shape[1:])
    spread = (ordered[0] + ordered[1] + ordered[2] + ordered[3])[0:1] / (members - 1)
    innovation = values[...] - mean
    place = tiles[...]
    rows = split_rows(innovation) + split_rows(error[...]) + split_rows(spread)
    rows += [(place // 32).astype(F32).astype(BF16), (place % 32).astype(F32).astype(BF16)]
    rows += [jnp.zeros((1, obs), BF16)] * (16 - len(rows))
    packet[members:] = jnp.concatenate(rows, axis=0)
    above = jnp.sum(innovation * innovation)
    below = jnp.sum(spread + error[...])
    lane = lax.broadcasted_iota(jnp.int32, sums.shape, 1)
    sums[...] = jnp.where(lane == 0, above, jnp.where(lane == 1, below, 0.0))


def stats(me, gathered, values, error, tiles, regions):
    peers = len(gathered)
    own, obs = gathered[0].shape
    return pl.pallas_call(
        stats_body,
        in_specs=[scalars()] + [whole()] * (3 + peers),
        out_specs=[whole(), whole()],
        out_shape=[shape_of((peers * own + 16, obs)), shape_of((regions, 128), F32)],
        scratch_shapes=[pltpu.VMEM((peers, 8, obs), F32)],
        compiler_params=params(),
        name="stats",
    )(me, values, error, tiles, *gathered)


def scalar_rows(rows):
    rows = rows.astype(F32)
    innovation = rows[0:1] + rows[1:2] + rows[2:3]
    error = rows[3:4] + rows[4:5] + rows[5:6]
    spread = rows[6:7] + rows[7:8] + rows[8:9]
    return innovation, error, spread, rows[9:10] * 32.0 + rows[10:11]


def gains(state, anom_t, taper, means, anomalies, gain):
    own = state[0].shape[0]
    parts = [part.astype(F32) for part in state]
    mean = sum(jnp.sum(part, axis=0, keepdims=True) for part in parts) / (own * len(parts))
    means[...] = jnp.broadcast_to(mean, means.shape)
    for s, part in enumerate(parts):
        anomalies[s * own : (s + 1) * own] = (part - mean).astype(BF16)
    at = 0
    for some_t in anom_t:
        rows = slice(at, at + some_t.shape[0])
        covariance = jnp.dot(some_t[...], anomalies[...], preferred_element_type=F32)
        gain[rows] = (covariance * taper[rows]).astype(BF16)
        at = rows.stop


def posterior(gain, means, anomalies, perturbed, root, blocks, at):
    own = blocks[0].shape[1]
    increment = jnp.dot(perturbed[...], gain[...], preferred_element_type=F32)
    result = means[0:1] + root * anomalies[...].astype(F32) + increment
    for s, block in enumerate(blocks):
        block[at] = result[s * own : (s + 1) * own].astype(BF16)


def tapers(scales, offset, taper, members, tile_count):
    width = taper.shape[1]
    tile = (offset[0] + lax.broadcasted_iota(jnp.int32, (1, width), 1)).astype(F32)
    places = [
        scalar_rows(rows)[3] + (offset[1 + n] * tile_count).astype(F32)
        for n, rows in enumerate(scales)
    ]
    obs = places[0].shape[1]
    columns = jnp.concatenate([*places, jnp.zeros((8 - len(places), obs), F32)], axis=0).T
    for n in range(len(places)):
        near = jnp.maximum(0.0, 1.0 - jnp.abs(tile - columns[:, n : n + 1]) * (1.0 / RADIUS))
        taper[n * obs : (n + 1) * obs] = near * near * (1.0 / (members - 1))


def prepare_body(*refs):
    *packets, anom_t = refs
    members = anom_t.shape[1]
    obs = packets[0].shape[1]
    for n, packet in enumerate(packets):
        anom_t[n * obs : (n + 1) * obs] = packet[:members].T


def prepare(packets):
    rows, obs = packets[0].shape
    members = rows - 16
    count = len(packets)
    return pl.pallas_call(
        prepare_body,
        in_specs=[whole()] * count,
        out_specs=whole(),
        out_shape=shape_of((count * obs, members)),
        compiler_params=params(4),
        name="prepare",
    )(*in_vmem(packets))


def start_body(offset, *refs, peers, tile_count):
    far_states, far_packets, far = refs[:peers], refs[peers : peers + 2], refs[peers + 2]
    anom_0, anom_2, taper, means, anomalies, gain, packets, rest = refs[peers + 3 : peers + 11]
    states, arrived, near, passed = refs[peers + 11 :]
    members = anomalies.shape[1]
    count = gain.shape[0]
    loads = [
        pltpu.make_async_copy(far_states[s].at[:count], states.at[s], arrived.at[s])
        for s in range(peers)
    ]
    late = [
        pltpu.make_async_copy(packet, packets.at[n], near.at[n])
        for n, packet in enumerate(far_packets)
    ]
    onward = [
        pltpu.make_async_copy(far_states[s].at[count:], rest.at[s], passed.at[s])
        for s in range(peers)
    ]
    for load in [*late, *loads, *onward]:
        load.start()
    anom_2[...] = far[:members].T
    for load in late:
        load.wait()
    rows = packets[0, members:], packets[1, members:], far[members:]
    tapers(rows, offset, taper, members, tile_count)
    for load in loads:
        load.wait()
    for l in range(count):
        state = [states[s, l] for s in range(peers)]
        gains(state, (anom_0, anom_2), taper, means.at[l], anomalies.at[l], gain.at[l])
    for load in onward:
        load.wait()


def start_gains(offset, states, packets, anom_0, count, tile_count):
    var_count, own, width = states[0].shape
    peers = len(states)
    members = own * peers
    rows, obs = packets[0].shape
    return pl.pallas_call(
        functools.partial(start_body, peers=peers, tile_count=tile_count),
        in_specs=[scalars()] + [anywhere()] * (peers + 2) + [whole()] * 2,
        out_specs=[whole()] * 7,
        out_shape=[
            shape_of((obs, members)),
            shape_of((3 * obs, width), F32),
            shape_of((count, 8, width), F32),
            shape_of((count, members, width)),
            shape_of((count, 3 * obs, width)),
            shape_of((2, rows, obs)),
            shape_of((peers, var_count - count, own, width)),
        ],
        scratch_shapes=[
            pltpu.VMEM((peers, count, own, width), BF16),
            pltpu.SemaphoreType.DMA((peers,)),
            pltpu.SemaphoreType.DMA((2,)),
            pltpu.SemaphoreType.DMA((peers,)),
        ],
        compiler_params=params(8),
        name="start",
    )(
        offset,
        in_hbm(states[0]),
        *states[1:],
        *map(in_hbm, packets[:2]),
        *in_vmem((packets[2], anom_0)),
    )


def first_body(means, anomalies, gain, packets, far, sums, noise_0, noise_1, noise_2, *refs):
    *blocks, perturbed, root_out, inflation_out = refs
    members = anomalies.shape[1]
    obs = packets.shape[2]
    folded = jnp.sum(sums[...], axis=0, keepdims=True)
    inflation = folded[:, 0:1] / folded[:, 1:2]
    inflation_out[0] = jnp.sum(inflation)
    root = jnp.sqrt(inflation)
    root_out[...] = jnp.broadcast_to(root, root_out.shape)
    for n, noise in enumerate((noise_0, noise_1, noise_2)):
        packet = far if n == 2 else packets.at[n]
        innovation, error, spread, _ = scalar_rows(packet[members:])
        bottom = jnp.where(error > 0.0, inflation * spread + error, 1.0)
        factor = jnp.where(error > 0.0, inflation / bottom, 0.0)
        dev = packet[:members].astype(F32)
        perturbed[:, n * obs : (n + 1) * obs] = (
            factor * (innovation + noise[...].astype(F32) - root * dev)
        ).astype(BF16)
    for l in range(gain.shape[0]):
        posterior(gain.at[l], means.at[l], anomalies.at[l], perturbed, root, blocks, l)


def working(count, members, obs, width):
    return [
        pltpu.VMEM((count, 8, width), F32),
        pltpu.VMEM((count, members, width), BF16),
        pltpu.VMEM((count, obs, width), BF16),
    ]


def first_updates(means, anomalies, gain, packets, far, sums, noises, peers):
    count, members, width = anomalies.shape
    obs = packets.shape[2]
    out = pl.pallas_call(
        first_body,
        in_specs=[whole()] * 9,
        out_specs=[whole()] * (peers + 2) + [scalars()],
        out_shape=[shape_of((count, members // peers, width))] * peers
        + [
            shape_of((members, 3 * obs)),
            shape_of((8, 128), F32),
            jax.ShapeDtypeStruct((1,), F32),
        ],
        compiler_params=params(4),
        name="first",
    )(*in_vmem((means, anomalies, gain, packets, far, sums, *noises)))
    return out[:peers], *out[peers:]


def second_body(states, perturbed, root, anom_0, anom_2, taper, *refs):
    *blocks, means, anomalies, gain = refs
    peers = len(blocks)
    count = blocks[0].shape[0]
    for l in range(count):
        state = [states[s, l] for s in range(peers)]
        gains(state, (anom_0, anom_2), taper, means.at[l], anomalies.at[l], gain.at[l])
    for l in range(count):
        posterior(gain.at[l], means.at[l], anomalies.at[l], perturbed, root[0:1, 0:1], blocks, l)


def second_updates(states, perturbed, root, shared):
    peers, count, own, width = states.shape
    return pl.pallas_call(
        second_body,
        in_specs=[whole()] * 6,
        out_specs=[whole()] * peers,
        out_shape=[shape_of((count, own, width))] * peers,
        scratch_shapes=working(count, peers * own, perturbed.shape[1], width),
        compiler_params=params(),
        name="second",
    )(*in_vmem((states, perturbed, root, *shared)))


def place_body(me, *refs, first, peers):
    blocks, out, done = refs[:peers], refs[-2], refs[-1]
    count, _, width = blocks[0].shape
    copies = [
        pltpu.make_async_copy(
            blocks[s],
            out.at[first : first + count, :, pl.ds(tile_block(me[0], s, width), width)],
            done.at[s],
        )
        for s in range(peers)
    ]
    for copy in copies:
        copy.start()
    for copy in copies:
        copy.wait()


def place(me, blocks, first, var_count, before=None):
    peers = len(blocks)
    _, own, width = blocks[0].shape
    more = [] if before is None else [before]
    return pl.pallas_call(
        functools.partial(place_body, first=first, peers=peers),
        in_specs=[scalars()] + [anywhere()] * (peers + len(more)),
        out_specs=anywhere(),
        out_shape=pltpu.HBM((var_count, own, peers * width), BF16),
        scratch_shapes=[pltpu.SemaphoreType.DMA((peers,))],
        input_output_aliases={1 + peers: 0} if more else {},
        compiler_params=params(),
    )(me, *in_vmem(blocks), *more)


def swapped(value, axis, distance):
    pairs = [(i, i ^ distance) for i in range(lax.axis_size(axis))]
    return lax.ppermute(value, axis, pairs)


def exchanged(blocks, axis):
    return lax.all_to_all(blocks, axis, split_axis=0, concat_axis=0, tiled=True)


def traded(blocks, order):
    out = list(blocks)
    for s in order:
        out[s] = swapped(blocks[s], "member", s)
    return out


def shards(ensemble, obs_weights, obs_tiles, obs_values, obs_error, obs_noise):
    peers = lax.axis_size("member")
    regions = lax.axis_size("region")
    var_count, _, tile_count = ensemble.shape
    width = tile_count // peers
    me = lax.axis_index("member").astype(jnp.int32)[None]
    region = lax.axis_index("region").astype(jnp.int32)
    tiles, values, error = (a[None, :] for a in (obs_tiles, obs_values, obs_error))
    *blocks, partial = pack(me, ensemble, obs_weights, tiles, peers)
    other = swapped(partial, "depth", 1)
    noises = traded([scale(obs_noise, error)] * peers, (1, 3, 2))
    predicted = traded([join(partial, other)] * peers, (1, 3, 2))
    pairs = [(i, i + 1) for i in range(1, regions - 1, 2)]
    pairs += [(j, i) for i, j in pairs]
    packet, sums = stats(me, predicted, values, error, tiles, regions)
    near = swapped(packet, "region", 1)
    far = lax.ppermute(packet, "region", pairs)
    states = traded(blocks, (1, 3, 2))
    all_sums = exchanged(sums, "region")
    noise = join_noise(noises)
    near_noise = swapped(noise, "region", 1)
    far_noise = lax.ppermute(noise, "region", pairs)
    side = 1 - 2 * (region % 2)
    offset = jnp.stack([me[0] * width, jnp.zeros_like(side), side, -side])
    anom_0 = prepare((packet, near))
    half = (var_count + 1) // 2
    anom_2, taper, means, anomalies, gain, packets, rest = start_gains(
        offset, states, (packet, near, far), anom_0, half, tile_count
    )
    ready, perturbed, root, inflation = first_updates(
        means, anomalies, gain, packets, far, all_sums, (noise, near_noise, far_noise), peers
    )
    shared = (anom_0, anom_2, taper)
    early = traded(ready, (1, 3, 2))
    ready = second_updates(rest, perturbed, root, shared)
    late = traded(ready, (1, 3, 2))
    output = place(me, early, 0, var_count)
    output = place(me, late, half, var_count, output)
    return (output, inflation.reshape(()))


def solution(mesh):
    return jax.shard_map(
        shards,
        mesh=mesh,
        in_specs=(
            P("depth", "member", "region"),
            P("depth"),
            P("region"),
            P("region"),
            P("region"),
            P("member", "region"),
        ),
        out_specs=(P("depth", "member", "region"), P()),
        check_vma=False,
    )
```

```python
import functools

import jax
import jax.numpy as jnp
from jax import lax
from jax.experimental import pallas as pl
from jax.experimental.pallas import tpu as pltpu
from jax.sharding import PartitionSpec as P


RADIUS = 1024
F32 = jnp.float32
BF16 = jnp.bfloat16


def params(megabytes=12):
    return pltpu.CompilerParams(vmem_limit_bytes=megabytes * 2**20)


def whole():
    return pl.BlockSpec(memory_space=pltpu.VMEM)


def scalars():
    return pl.BlockSpec(memory_space=pltpu.SMEM)


def anywhere():
    return pl.BlockSpec(memory_space=pl.ANY)


def shape_of(shape, dtype=BF16):
    return pltpu.VMEM(shape, dtype)


def in_vmem(values):
    return [pltpu.with_memory_space_constraint(v, pltpu.VMEM) for v in values]


def in_hbm(value):
    return pltpu.with_memory_space_constraint(value, pltpu.HBM)


def split_rows(value):
    first = value.astype(BF16)
    rest = value - first.astype(F32)
    second = rest.astype(BF16)
    third = (rest - second.astype(F32)).astype(BF16)
    return [first, second, third]


def tile_block(me, s, width):
    return pl.multiple_of(jnp.bitwise_xor(me, s) * width, width)


def pack_body(me, far_weights, ensemble, far_tiles, *rest):
    *blocks, predicted, weights, tiles, chosen, halves, buffer, arrived, left = rest
    peers, var_count, _, width = buffer.shape
    starts = [tile_block(me[0], s, width) for s in range(peers)]
    loads = [
        pltpu.make_async_copy(
            ensemble.at[:, :, pl.ds(starts[s], width)], buffer.at[s], arrived.at[s]
        )
        for s in range(peers)
    ]
    stores = [pltpu.make_async_copy(buffer.at[s], blocks[s], left.at[s]) for s in range(peers)]
    light = [
        pltpu.make_async_copy(far_weights, weights, arrived.at[peers]),
        pltpu.make_async_copy(far_tiles, tiles, arrived.at[peers + 1]),
    ]
    for load in light + loads:
        load.start()
    for load in light:
        load.wait()
    rows = lax.broadcasted_iota(jnp.int32, (width, tiles.shape[1]), 0)
    for s in range(peers):
        chosen[s * width : (s + 1) * width] = jnp.where(
            tiles[...] - starts[s] == rows, 1.0, 0.0
        ).astype(BF16)
    for s in range(peers):
        loads[s].wait()
        stores[s].start()
        mixed = weights[0] * buffer[s, 0].astype(F32)
        for l in range(1, var_count):
            mixed = mixed + weights[l] * buffer[s, l].astype(F32)
        high = mixed.astype(BF16)
        columns = slice(s * width, (s + 1) * width)
        halves[: mixed.shape[0], columns] = high
        halves[mixed.shape[0] :, columns] = (mixed - high.astype(F32)).astype(BF16)
    picked = jnp.dot(halves[...], chosen[...], preferred_element_type=F32)
    own = predicted.shape[0]
    predicted[...] = (picked[:own] + picked[own:]).astype(BF16)
    for store in stores:
        store.wait()


def pack(me, ensemble, weights, tiles, peers):
    var_count, own, tile_count = ensemble.shape
    width = tile_count // peers
    obs = tiles.shape[1]
    return pl.pallas_call(
        pack_body,
        in_specs=[scalars()] + [anywhere()] * 3,
        out_specs=[anywhere()] * peers + [whole()],
        out_shape=[pltpu.HBM((var_count, own, width), BF16)] * peers + [shape_of((own, obs))],
        scratch_shapes=[
            pltpu.SMEM((var_count,), F32),
            pltpu.VMEM((1, obs), jnp.int32),
            pltpu.VMEM((tile_count, obs), BF16),
            pltpu.VMEM((2 * own, tile_count), BF16),
            pltpu.VMEM((peers, var_count, own, width), BF16),
            pltpu.SemaphoreType.DMA((peers + 2,)),
            pltpu.SemaphoreType.DMA((peers,)),
        ],
        compiler_params=params(),
        name="pack",
    )(me, in_hbm(weights), in_hbm(ensemble), in_hbm(tiles))


def scale_body(noise, error, out):
    out[...] = (jnp.sqrt(error[...]) * noise[...]).astype(BF16)


def scale(noise, error):
    return pl.pallas_call(
        scale_body,
        in_specs=[whole()] * 2,
        out_specs=whole(),
        out_shape=shape_of(noise.shape),
        compiler_params=params(),
        name="scale",
    )(noise, error)


def join_noise_body(*refs):
    *parts, out = refs
    own = parts[0].shape[0]
    for s, part in enumerate(parts):
        out[s * own : (s + 1) * own] = part[...]


def join_noise(parts):
    own, obs = parts[0].shape
    return pl.pallas_call(
        join_noise_body,
        in_specs=[whole()] * len(parts),
        out_specs=whole(),
        out_shape=shape_of((len(parts) * own, obs)),
        compiler_params=params(),
        name="joinnoise",
    )(*parts)


def join_body(mine, other, out):
    out[...] = (mine[...].astype(F32) + other[...].astype(F32)).astype(BF16)


def join(mine, other):
    return pl.pallas_call(
        join_body,
        in_specs=[whole()] * 2,
        out_specs=whole(),
        out_shape=shape_of(mine.shape),
        compiler_params=params(),
        name="join",
    )(mine, other)


def stats_body(me, values, error, tiles, *refs):
    *gathered, packet, sums, ordered = refs
    peers = len(gathered)
    own, obs = gathered[0].shape
    members = peers * own
    for s in range(peers):
        part = jnp.sum(gathered[s][...].astype(F32), axis=0, keepdims=True)
        ordered[jnp.bitwise_xor(me[0], s)] = jnp.broadcast_to(part, ordered.shape[1:])
    mean = (ordered[0] + ordered[1] + ordered[2] + ordered[3])[0:1] / members
    for s in range(peers):
        dev = gathered[s][...].astype(F32) - mean
        packet[s * own : (s + 1) * own] = dev.astype(BF16)
        part = jnp.sum(dev * dev, axis=0, keepdims=True)
        ordered[jnp.bitwise_xor(me[0], s)] = jnp.broadcast_to(part, ordered.shape[1:])
    spread = (ordered[0] + ordered[1] + ordered[2] + ordered[3])[0:1] / (members - 1)
    innovation = values[...] - mean
    place = tiles[...]
    rows = split_rows(innovation) + split_rows(error[...]) + split_rows(spread)
    rows += [(place // 32).astype(F32).astype(BF16), (place % 32).astype(F32).astype(BF16)]
    rows += [jnp.zeros((1, obs), BF16)] * (16 - len(rows))
    packet[members:] = jnp.concatenate(rows, axis=0)
    above = jnp.sum(innovation * innovation)
    below = jnp.sum(spread + error[...])
    lane = lax.broadcasted_iota(jnp.int32, sums.shape, 1)
    sums[...] = jnp.where(lane == 0, above, jnp.where(lane == 1, below, 0.0))


def stats(me, gathered, values, error, tiles, regions):
    peers = len(gathered)
    own, obs = gathered[0].shape
    return pl.pallas_call(
        stats_body,
        in_specs=[scalars()] + [whole()] * (3 + peers),
        out_specs=[whole(), whole()],
        out_shape=[shape_of((peers * own + 16, obs)), shape_of((regions, 128), F32)],
        scratch_shapes=[pltpu.VMEM((peers, 8, obs), F32)],
        compiler_params=params(),
        name="stats",
    )(me, values, error, tiles, *gathered)


def scalar_rows(rows):
    rows = rows.astype(F32)
    innovation = rows[0:1] + rows[1:2] + rows[2:3]
    error = rows[3:4] + rows[4:5] + rows[5:6]
    spread = rows[6:7] + rows[7:8] + rows[8:9]
    return innovation, error, spread, rows[9:10] * 32.0 + rows[10:11]


def gains(state, anom_t, taper, means, anomalies, gain):
    own = state[0].shape[0]
    parts = [part.astype(F32) for part in state]
    mean = sum(jnp.sum(part, axis=0, keepdims=True) for part in parts) / (own * len(parts))
    means[...] = jnp.broadcast_to(mean, means.shape)
    for s, part in enumerate(parts):
        anomalies[s * own : (s + 1) * own] = (part - mean).astype(BF16)
    at = 0
    for some_t in anom_t:
        rows = slice(at, at + some_t.shape[0])
        covariance = jnp.dot(some_t[...], anomalies[...], preferred_element_type=F32)
        gain[rows] = (covariance * taper[rows]).astype(BF16)
        at = rows.stop


def posterior(gain, means, anomalies, perturbed, root, blocks, at):
    own = blocks[0].shape[1]
    increment = jnp.dot(perturbed[...], gain[...], preferred_element_type=F32)
    result = means[0:1] + root * anomalies[...].astype(F32) + increment
    for s, block in enumerate(blocks):
        block[at] = result[s * own : (s + 1) * own].astype(BF16)


def tapers(scales, offset, taper, members, tile_count):
    width = taper.shape[1]
    tile = (offset[0] + lax.broadcasted_iota(jnp.int32, (1, width), 1)).astype(F32)
    places = [
        scalar_rows(rows)[3] + (offset[1 + n] * tile_count).astype(F32)
        for n, rows in enumerate(scales)
    ]
    obs = places[0].shape[1]
    columns = jnp.concatenate([*places, jnp.zeros((8 - len(places), obs), F32)], axis=0).T
    for n in range(len(places)):
        near = jnp.maximum(0.0, 1.0 - jnp.abs(tile - columns[:, n : n + 1]) * (1.0 / RADIUS))
        taper[n * obs : (n + 1) * obs] = near * near * (1.0 / (members - 1))


def prepare_body(*refs):
    *packets, anom_t = refs
    members = anom_t.shape[1]
    obs = packets[0].shape[1]
    for n, packet in enumerate(packets):
        anom_t[n * obs : (n + 1) * obs] = packet[:members].T


def prepare(packets):
    rows, obs = packets[0].shape
    members = rows - 16
    count = len(packets)
    return pl.pallas_call(
        prepare_body,
        in_specs=[whole()] * count,
        out_specs=whole(),
        out_shape=shape_of((count * obs, members)),
        compiler_params=params(4),
        name="prepare",
    )(*in_vmem(packets))


def start_body(offset, *refs, peers, tile_count):
    far_states, far_packets, far = refs[:peers], refs[peers : peers + 2], refs[peers + 2]
    anom_0, anom_2, taper, means, anomalies, gain, packets, rest = refs[peers + 3 : peers + 11]
    states, arrived, near, passed = refs[peers + 11 :]
    members = anomalies.shape[1]
    count = gain.shape[0]
    loads = [
        pltpu.make_async_copy(far_states[s].at[:count], states.at[s], arrived.at[s])
        for s in range(peers)
    ]
    light = [
        pltpu.make_async_copy(packet.at[members:], packets.at[n, members:], near.at[n])
        for n, packet in enumerate(far_packets)
    ]
    late = [
        pltpu.make_async_copy(packet.at[:members], packets.at[n, :members], near.at[2 + n])
        for n, packet in enumerate(far_packets)
    ]
    onward = [
        pltpu.make_async_copy(far_states[s].at[count:], rest.at[s], passed.at[s])
        for s in range(peers)
    ]
    for load in [*light, *loads, *late, *onward]:
        load.start()
    anom_2[...] = far[:members].T
    for load in light:
        load.wait()
    rows = packets[0, members:], packets[1, members:], far[members:]
    tapers(rows, offset, taper, members, tile_count)
    for load in loads:
        load.wait()
    for l in range(count):
        state = [states[s, l] for s in range(peers)]
        gains(state, (anom_0, anom_2), taper, means.at[l], anomalies.at[l], gain.at[l])
    for load in [*late, *onward]:
        load.wait()


def start_gains(offset, states, packets, anom_0, count, tile_count):
    var_count, own, width = states[0].shape
    peers = len(states)
    members = own * peers
    rows, obs = packets[0].shape
    return pl.pallas_call(
        functools.partial(start_body, peers=peers, tile_count=tile_count),
        in_specs=[scalars()] + [anywhere()] * (peers + 2) + [whole()] * 2,
        out_specs=[whole()] * 7,
        out_shape=[
            shape_of((obs, members)),
            shape_of((3 * obs, width), F32),
            shape_of((count, 8, width), F32),
            shape_of((count, members, width)),
            shape_of((count, 3 * obs, width)),
            shape_of((2, rows, obs)),
            shape_of((peers, var_count - count, own, width)),
        ],
        scratch_shapes=[
            pltpu.VMEM((peers, count, own, width), BF16),
            pltpu.SemaphoreType.DMA((peers,)),
            pltpu.SemaphoreType.DMA((4,)),
            pltpu.SemaphoreType.DMA((peers,)),
        ],
        compiler_params=params(8),
        name="start",
    )(
        offset,
        in_hbm(states[0]),
        *states[1:],
        *map(in_hbm, packets[:2]),
        *in_vmem((packets[2], anom_0)),
    )


def first_body(means, anomalies, gain, packets, far, sums, noise_0, noise_1, noise_2, *refs):
    *blocks, perturbed, root_out, inflation_out = refs
    members = anomalies.shape[1]
    obs = packets.shape[2]
    folded = jnp.sum(sums[...], axis=0, keepdims=True)
    inflation = folded[:, 0:1] / folded[:, 1:2]
    inflation_out[0] = jnp.sum(inflation)
    root = jnp.sqrt(inflation)
    root_out[...] = jnp.broadcast_to(root, root_out.shape)
    for n, noise in enumerate((noise_0, noise_1, noise_2)):
        packet = far if n == 2 else packets.at[n]
        innovation, error, spread, _ = scalar_rows(packet[members:])
        bottom = jnp.where(error > 0.0, inflation * spread + error, 1.0)
        factor = jnp.where(error > 0.0, inflation / bottom, 0.0)
        dev = packet[:members].astype(F32)
        perturbed[:, n * obs : (n + 1) * obs] = (
            factor * (innovation + noise[...].astype(F32) - root * dev)
        ).astype(BF16)
    for l in range(gain.shape[0]):
        posterior(gain.at[l], means.at[l], anomalies.at[l], perturbed, root, blocks, l)


def working(count, members, obs, width):
    return [
        pltpu.VMEM((count, 8, width), F32),
        pltpu.VMEM((count, members, width), BF16),
        pltpu.VMEM((count, obs, width), BF16),
    ]


def first_updates(means, anomalies, gain, packets, far, sums, noises, peers):
    count, members, width = anomalies.shape
    obs = packets.shape[2]
    out = pl.pallas_call(
        first_body,
        in_specs=[whole()] * 9,
        out_specs=[whole()] * (peers + 2) + [scalars()],
        out_shape=[shape_of((count, members // peers, width))] * peers
        + [
            shape_of((members, 3 * obs)),
            shape_of((8, 128), F32),
            jax.ShapeDtypeStruct((1,), F32),
        ],
        compiler_params=params(4),
        name="first",
    )(*in_vmem((means, anomalies, gain, packets, far, sums, *noises)))
    return out[:peers], *out[peers:]


def second_body(states, perturbed, root, anom_0, anom_2, taper, *refs):
    *blocks, means, anomalies, gain = refs
    peers = len(blocks)
    count = blocks[0].shape[0]
    for l in range(count):
        state = [states[s, l] for s in range(peers)]
        gains(state, (anom_0, anom_2), taper, means.at[l], anomalies.at[l], gain.at[l])
    for l in range(count):
        posterior(gain.at[l], means.at[l], anomalies.at[l], perturbed, root[0:1, 0:1], blocks, l)


def second_updates(states, perturbed, root, shared):
    peers, count, own, width = states.shape
    return pl.pallas_call(
        second_body,
        in_specs=[whole()] * 6,
        out_specs=[whole()] * peers,
        out_shape=[shape_of((count, own, width))] * peers,
        scratch_shapes=working(count, peers * own, perturbed.shape[1], width),
        compiler_params=params(),
        name="second",
    )(*in_vmem((states, perturbed, root, *shared)))


def place_body(me, *refs, first, peers):
    blocks, out, done = refs[:peers], refs[-2], refs[-1]
    count, _, width = blocks[0].shape
    copies = [
        pltpu.make_async_copy(
            blocks[s],
            out.at[first : first + count, :, pl.ds(tile_block(me[0], s, width), width)],
            done.at[s],
        )
        for s in range(peers)
    ]
    for copy in copies:
        copy.start()
    for copy in copies:
        copy.wait()


def place(me, blocks, first, var_count, before=None):
    peers = len(blocks)
    _, own, width = blocks[0].shape
    more = [] if before is None else [before]
    return pl.pallas_call(
        functools.partial(place_body, first=first, peers=peers),
        in_specs=[scalars()] + [anywhere()] * (peers + len(more)),
        out_specs=anywhere(),
        out_shape=pltpu.HBM((var_count, own, peers * width), BF16),
        scratch_shapes=[pltpu.SemaphoreType.DMA((peers,))],
        input_output_aliases={1 + peers: 0} if more else {},
        compiler_params=params(),
    )(me, *in_vmem(blocks), *more)


def swapped(value, axis, distance):
    pairs = [(i, i ^ distance) for i in range(lax.axis_size(axis))]
    return lax.ppermute(value, axis, pairs)


def exchanged(blocks, axis):
    return lax.all_to_all(blocks, axis, split_axis=0, concat_axis=0, tiled=True)


def traded(blocks, order):
    out = list(blocks)
    for s in order:
        out[s] = swapped(blocks[s], "member", s)
    return out


def shards(ensemble, obs_weights, obs_tiles, obs_values, obs_error, obs_noise):
    peers = lax.axis_size("member")
    regions = lax.axis_size("region")
    var_count, _, tile_count = ensemble.shape
    width = tile_count // peers
    me = lax.axis_index("member").astype(jnp.int32)[None]
    region = lax.axis_index("region").astype(jnp.int32)
    tiles, values, error = (a[None, :] for a in (obs_tiles, obs_values, obs_error))
    *blocks, partial = pack(me, ensemble, obs_weights, tiles, peers)
    other = swapped(partial, "depth", 1)
    noises = traded([scale(obs_noise, error)] * peers, (1, 3, 2))
    predicted = traded([join(partial, other)] * peers, (1, 3, 2))
    pairs = [(i, i + 1) for i in range(1, regions - 1, 2)]
    pairs += [(j, i) for i, j in pairs]
    packet, sums = stats(me, predicted, values, error, tiles, regions)
    near = swapped(packet, "region", 1)
    far = lax.ppermute(packet, "region", pairs)
    states = traded(blocks, (1, 3, 2))
    all_sums = exchanged(sums, "region")
    noise = join_noise(noises)
    near_noise = swapped(noise, "region", 1)
    far_noise = lax.ppermute(noise, "region", pairs)
    side = 1 - 2 * (region % 2)
    offset = jnp.stack([me[0] * width, jnp.zeros_like(side), side, -side])
    anom_0 = prepare((packet, near))
    half = (var_count + 1) // 2
    anom_2, taper, means, anomalies, gain, packets, rest = start_gains(
        offset, states, (packet, near, far), anom_0, half, tile_count
    )
    ready, perturbed, root, inflation = first_updates(
        means, anomalies, gain, packets, far, all_sums, (noise, near_noise, far_noise), peers
    )
    shared = (anom_0, anom_2, taper)
    early = traded(ready, (1, 3, 2))
    ready = second_updates(rest, perturbed, root, shared)
    late = traded(ready, (1, 3, 2))
    output = place(me, early, 0, var_count)
    output = place(me, late, half, var_count, output)
    return (output, inflation.reshape(()))


def solution(mesh):
    return jax.shard_map(
        shards,
        mesh=mesh,
        in_specs=(
            P("depth", "member", "region"),
            P("depth"),
            P("region"),
            P("region"),
            P("region"),
            P("member", "region"),
        ),
        out_specs=(P("depth", "member", "region"), P()),
        check_vma=False,
    )
```

```python
import functools

import jax
import jax.numpy as jnp
from jax import lax
from jax.experimental import pallas as pl
from jax.experimental.pallas import tpu as pltpu
from jax.sharding import PartitionSpec as P


RADIUS = 1024
F32 = jnp.float32
BF16 = jnp.bfloat16


def params(megabytes=12):
    return pltpu.CompilerParams(vmem_limit_bytes=megabytes * 2**20)


def whole():
    return pl.BlockSpec(memory_space=pltpu.VMEM)


def scalars():
    return pl.BlockSpec(memory_space=pltpu.SMEM)


def anywhere():
    return pl.BlockSpec(memory_space=pl.ANY)


def shape_of(shape, dtype=BF16):
    return pltpu.VMEM(shape, dtype)


def in_vmem(values):
    return [pltpu.with_memory_space_constraint(v, pltpu.VMEM) for v in values]


def in_hbm(value):
    return pltpu.with_memory_space_constraint(value, pltpu.HBM)


def split_rows(value):
    first = value.astype(BF16)
    rest = value - first.astype(F32)
    second = rest.astype(BF16)
    third = (rest - second.astype(F32)).astype(BF16)
    return [first, second, third]


def tile_block(me, s, width):
    return pl.multiple_of(jnp.bitwise_xor(me, s) * width, width)


def pack_body(me, far_weights, ensemble, far_tiles, *rest):
    *blocks, predicted, weights, tiles, chosen, halves, buffer, arrived, left = rest
    peers, var_count, _, width = buffer.shape
    starts = [tile_block(me[0], s, width) for s in range(peers)]
    loads = [
        pltpu.make_async_copy(
            ensemble.at[:, :, pl.ds(starts[s], width)], buffer.at[s], arrived.at[s]
        )
        for s in range(peers)
    ]
    stores = [
        pltpu.make_async_copy(buffer.at[s], blocks[s - 1], left.at[s]) for s in range(1, peers)
    ]
    light = [
        pltpu.make_async_copy(far_weights, weights, arrived.at[peers]),
        pltpu.make_async_copy(far_tiles, tiles, arrived.at[peers + 1]),
    ]
    for load in light + loads:
        load.start()
    for load in light:
        load.wait()
    rows = lax.broadcasted_iota(jnp.int32, (width, tiles.shape[1]), 0)
    for s in range(peers):
        chosen[s * width : (s + 1) * width] = jnp.where(
            tiles[...] - starts[s] == rows, 1.0, 0.0
        ).astype(BF16)
    for s in range(peers):
        loads[s].wait()
        if s:
            stores[s - 1].start()
        mixed = weights[0] * buffer[s, 0].astype(F32)
        for l in range(1, var_count):
            mixed = mixed + weights[l] * buffer[s, l].astype(F32)
        high = mixed.astype(BF16)
        columns = slice(s * width, (s + 1) * width)
        halves[: mixed.shape[0], columns] = high
        halves[mixed.shape[0] :, columns] = (mixed - high.astype(F32)).astype(BF16)
    picked = jnp.dot(halves[...], chosen[...], preferred_element_type=F32)
    own = predicted.shape[0]
    predicted[...] = (picked[:own] + picked[own:]).astype(BF16)
    for store in stores:
        store.wait()


def pack(me, ensemble, weights, tiles, peers):
    var_count, own, tile_count = ensemble.shape
    width = tile_count // peers
    obs = tiles.shape[1]
    return pl.pallas_call(
        pack_body,
        in_specs=[scalars()] + [anywhere()] * 3,
        out_specs=[anywhere()] * (peers - 1) + [whole()],
        out_shape=[pltpu.HBM((var_count, own, width), BF16)] * (peers - 1) + [shape_of((own, obs))],
        scratch_shapes=[
            pltpu.SMEM((var_count,), F32),
            pltpu.VMEM((1, obs), jnp.int32),
            pltpu.VMEM((tile_count, obs), BF16),
            pltpu.VMEM((2 * own, tile_count), BF16),
            pltpu.VMEM((peers, var_count, own, width), BF16),
            pltpu.SemaphoreType.DMA((peers + 2,)),
            pltpu.SemaphoreType.DMA((peers,)),
        ],
        compiler_params=params(),
        name="pack",
    )(me, in_hbm(weights), in_hbm(ensemble), in_hbm(tiles))


def scale_body(noise, error, out):
    out[...] = (jnp.sqrt(error[...]) * noise[...]).astype(BF16)


def scale(noise, error):
    return pl.pallas_call(
        scale_body,
        in_specs=[whole()] * 2,
        out_specs=whole(),
        out_shape=shape_of(noise.shape),
        compiler_params=params(),
        name="scale",
    )(noise, error)


def join_noise_body(*refs):
    *parts, out = refs
    own = parts[0].shape[0]
    for s, part in enumerate(parts):
        out[s * own : (s + 1) * own] = part[...]


def join_noise(parts):
    own, obs = parts[0].shape
    return pl.pallas_call(
        join_noise_body,
        in_specs=[whole()] * len(parts),
        out_specs=whole(),
        out_shape=shape_of((len(parts) * own, obs)),
        compiler_params=params(),
        name="joinnoise",
    )(*parts)


def join_body(mine, other, out):
    out[...] = (mine[...].astype(F32) + other[...].astype(F32)).astype(BF16)


def join(mine, other):
    return pl.pallas_call(
        join_body,
        in_specs=[whole()] * 2,
        out_specs=whole(),
        out_shape=shape_of(mine.shape),
        compiler_params=params(),
        name="join",
    )(mine, other)


def stats_body(me, values, error, tiles, *refs):
    *gathered, packet, sums, ordered = refs
    peers = len(gathered)
    own, obs = gathered[0].shape
    members = peers * own
    for s in range(peers):
        part = jnp.sum(gathered[s][...].astype(F32), axis=0, keepdims=True)
        ordered[jnp.bitwise_xor(me[0], s)] = jnp.broadcast_to(part, ordered.shape[1:])
    mean = (ordered[0] + ordered[1] + ordered[2] + ordered[3])[0:1] / members
    for s in range(peers):
        dev = gathered[s][...].astype(F32) - mean
        packet[s * own : (s + 1) * own] = dev.astype(BF16)
        part = jnp.sum(dev * dev, axis=0, keepdims=True)
        ordered[jnp.bitwise_xor(me[0], s)] = jnp.broadcast_to(part, ordered.shape[1:])
    spread = (ordered[0] + ordered[1] + ordered[2] + ordered[3])[0:1] / (members - 1)
    innovation = values[...] - mean
    place = tiles[...]
    rows = split_rows(innovation) + split_rows(error[...]) + split_rows(spread)
    rows += [(place // 32).astype(F32).astype(BF16), (place % 32).astype(F32).astype(BF16)]
    rows += [jnp.zeros((1, obs), BF16)] * (16 - len(rows))
    packet[members:] = jnp.concatenate(rows, axis=0)
    above = jnp.sum(innovation * innovation)
    below = jnp.sum(spread + error[...])
    lane = lax.broadcasted_iota(jnp.int32, sums.shape, 1)
    sums[...] = jnp.where(lane == 0, above, jnp.where(lane == 1, below, 0.0))


def stats(me, gathered, values, error, tiles, regions):
    peers = len(gathered)
    own, obs = gathered[0].shape
    return pl.pallas_call(
        stats_body,
        in_specs=[scalars()] + [whole()] * (3 + peers),
        out_specs=[whole(), whole()],
        out_shape=[shape_of((peers * own + 16, obs)), shape_of((regions, 128), F32)],
        scratch_shapes=[pltpu.VMEM((peers, 8, obs), F32)],
        compiler_params=params(),
        name="stats",
    )(me, values, error, tiles, *gathered)


def scalar_rows(rows):
    rows = rows.astype(F32)
    innovation = rows[0:1] + rows[1:2] + rows[2:3]
    error = rows[3:4] + rows[4:5] + rows[5:6]
    spread = rows[6:7] + rows[7:8] + rows[8:9]
    return innovation, error, spread, rows[9:10] * 32.0 + rows[10:11]


def gains(state, anom_t, taper, means, anomalies, gain):
    own = state[0].shape[0]
    parts = [part.astype(F32) for part in state]
    mean = sum(jnp.sum(part, axis=0, keepdims=True) for part in parts) / (own * len(parts))
    means[...] = jnp.broadcast_to(mean, means.shape)
    for s, part in enumerate(parts):
        anomalies[s * own : (s + 1) * own] = (part - mean).astype(BF16)
    at = 0
    for some_t in anom_t:
        rows = slice(at, at + some_t.shape[0])
        covariance = jnp.dot(some_t[...], anomalies[...], preferred_element_type=F32)
        gain[rows] = (covariance * taper[rows]).astype(BF16)
        at = rows.stop


def posterior(gain, means, anomalies, perturbed, root, blocks, at):
    own = blocks[0].shape[1]
    increment = jnp.dot(perturbed[...], gain[...], preferred_element_type=F32)
    result = means[0:1] + root * anomalies[...].astype(F32) + increment
    for s, block in enumerate(blocks):
        block[at] = result[s * own : (s + 1) * own].astype(BF16)


def tapers(scales, offset, taper, members, tile_count):
    width = taper.shape[1]
    tile = (offset[0] + lax.broadcasted_iota(jnp.int32, (1, width), 1)).astype(F32)
    places = [
        scalar_rows(rows)[3] + (offset[1 + n] * tile_count).astype(F32)
        for n, rows in enumerate(scales)
    ]
    obs = places[0].shape[1]
    columns = jnp.concatenate([*places, jnp.zeros((8 - len(places), obs), F32)], axis=0).T
    for n in range(len(places)):
        near = jnp.maximum(0.0, 1.0 - jnp.abs(tile - columns[:, n : n + 1]) * (1.0 / RADIUS))
        taper[n * obs : (n + 1) * obs] = near * near * (1.0 / (members - 1))


def prepare_body(*refs):
    *packets, anom_t = refs
    members = anom_t.shape[1]
    obs = packets[0].shape[1]
    for n, packet in enumerate(packets):
        anom_t[n * obs : (n + 1) * obs] = packet[:members].T


def prepare(packets):
    rows, obs = packets[0].shape
    members = rows - 16
    count = len(packets)
    return pl.pallas_call(
        prepare_body,
        in_specs=[whole()] * count,
        out_specs=whole(),
        out_shape=shape_of((count * obs, members)),
        compiler_params=params(4),
        name="prepare",
    )(*in_vmem(packets))


def start_body(offset, *refs, peers, tile_count):
    far_states, far_packets, far = refs[:peers], refs[peers : peers + 2], refs[peers + 2]
    anom_0, anom_2, taper, means, anomalies, gain, packets, rest = refs[peers + 3 : peers + 11]
    states, arrived, near, passed = refs[peers + 11 :]
    members = anomalies.shape[1]
    count = gain.shape[0]
    width = states.shape[3]
    own_tiles = far_states[0].at[:, :, pl.ds(pl.multiple_of(offset[0], width), width)]
    far_states = [own_tiles, *far_states[1:]]
    loads = [
        pltpu.make_async_copy(far_states[s].at[:count], states.at[s], arrived.at[s])
        for s in range(peers)
    ]
    late = [
        pltpu.make_async_copy(packet, packets.at[n], near.at[n])
        for n, packet in enumerate(far_packets)
    ]
    onward = [
        pltpu.make_async_copy(far_states[s].at[count:], rest.at[s], passed.at[s])
        for s in range(peers)
    ]
    for load in [*late, *loads, *onward]:
        load.start()
    anom_2[...] = far[:members].T
    for load in late:
        load.wait()
    rows = packets[0, members:], packets[1, members:], far[members:]
    tapers(rows, offset, taper, members, tile_count)
    for load in loads:
        load.wait()
    for l in range(count):
        state = [states[s, l] for s in range(peers)]
        gains(state, (anom_0, anom_2), taper, means.at[l], anomalies.at[l], gain.at[l])
    for load in onward:
        load.wait()


def start_gains(offset, states, packets, anom_0, count, tile_count):
    var_count, own, width = states[1].shape
    peers = len(states)
    members = own * peers
    rows, obs = packets[0].shape
    return pl.pallas_call(
        functools.partial(start_body, peers=peers, tile_count=tile_count),
        in_specs=[scalars()] + [anywhere()] * (peers + 2) + [whole()] * 2,
        out_specs=[whole()] * 7,
        out_shape=[
            shape_of((obs, members)),
            shape_of((3 * obs, width), F32),
            shape_of((count, 8, width), F32),
            shape_of((count, members, width)),
            shape_of((count, 3 * obs, width)),
            shape_of((2, rows, obs)),
            shape_of((peers, var_count - count, own, width)),
        ],
        scratch_shapes=[
            pltpu.VMEM((peers, count, own, width), BF16),
            pltpu.SemaphoreType.DMA((peers,)),
            pltpu.SemaphoreType.DMA((2,)),
            pltpu.SemaphoreType.DMA((peers,)),
        ],
        compiler_params=params(8),
        name="start",
    )(
        offset,
        in_hbm(states[0]),
        *states[1:],
        *map(in_hbm, packets[:2]),
        *in_vmem((packets[2], anom_0)),
    )


def first_body(means, anomalies, gain, packets, far, sums, noise_0, noise_1, noise_2, *refs):
    *blocks, perturbed, root_out, inflation_out = refs
    members = anomalies.shape[1]
    obs = packets.shape[2]
    folded = jnp.sum(sums[...], axis=0, keepdims=True)
    inflation = folded[:, 0:1] / folded[:, 1:2]
    inflation_out[0] = jnp.sum(inflation)
    root = jnp.sqrt(inflation)
    root_out[...] = jnp.broadcast_to(root, root_out.shape)
    for n, noise in enumerate((noise_0, noise_1, noise_2)):
        packet = far if n == 2 else packets.at[n]
        innovation, error, spread, _ = scalar_rows(packet[members:])
        bottom = jnp.where(error > 0.0, inflation * spread + error, 1.0)
        factor = jnp.where(error > 0.0, inflation / bottom, 0.0)
        dev = packet[:members].astype(F32)
        perturbed[:, n * obs : (n + 1) * obs] = (
            factor * (innovation + noise[...].astype(F32) - root * dev)
        ).astype(BF16)
    for l in range(gain.shape[0]):
        posterior(gain.at[l], means.at[l], anomalies.at[l], perturbed, root, blocks, l)


def working(count, members, obs, width):
    return [
        pltpu.VMEM((count, 8, width), F32),
        pltpu.VMEM((count, members, width), BF16),
        pltpu.VMEM((count, obs, width), BF16),
    ]


def first_updates(means, anomalies, gain, packets, far, sums, noises, peers):
    count, members, width = anomalies.shape
    obs = packets.shape[2]
    out = pl.pallas_call(
        first_body,
        in_specs=[whole()] * 9,
        out_specs=[whole()] * (peers + 2) + [scalars()],
        out_shape=[shape_of((count, members // peers, width))] * peers
        + [
            shape_of((members, 3 * obs)),
            shape_of((8, 128), F32),
            jax.ShapeDtypeStruct((1,), F32),
        ],
        compiler_params=params(4),
        name="first",
    )(*in_vmem((means, anomalies, gain, packets, far, sums, *noises)))
    return out[:peers], *out[peers:]


def second_body(states, perturbed, root, anom_0, anom_2, taper, *refs):
    *blocks, means, anomalies, gain = refs
    peers = len(blocks)
    count = blocks[0].shape[0]
    for l in range(count):
        state = [states[s, l] for s in range(peers)]
        gains(state, (anom_0, anom_2), taper, means.at[l], anomalies.at[l], gain.at[l])
    for l in range(count):
        posterior(gain.at[l], means.at[l], anomalies.at[l], perturbed, root[0:1, 0:1], blocks, l)


def second_updates(states, perturbed, root, shared):
    peers, count, own, width = states.shape
    return pl.pallas_call(
        second_body,
        in_specs=[whole()] * 6,
        out_specs=[whole()] * peers,
        out_shape=[shape_of((count, own, width))] * peers,
        scratch_shapes=working(count, peers * own, perturbed.shape[1], width),
        compiler_params=params(),
        name="second",
    )(*in_vmem((states, perturbed, root, *shared)))


def place_body(me, *refs, first, peers):
    blocks, out, done = refs[:peers], refs[-2], refs[-1]
    count, _, width = blocks[0].shape
    copies = [
        pltpu.make_async_copy(
            blocks[s],
            out.at[first : first + count, :, pl.ds(tile_block(me[0], s, width), width)],
            done.at[s],
        )
        for s in range(peers)
    ]
    for copy in copies:
        copy.start()
    for copy in copies:
        copy.wait()


def place(me, blocks, first, var_count, before=None):
    peers = len(blocks)
    _, own, width = blocks[0].shape
    more = [] if before is None else [before]
    return pl.pallas_call(
        functools.partial(place_body, first=first, peers=peers),
        in_specs=[scalars()] + [anywhere()] * (peers + len(more)),
        out_specs=anywhere(),
        out_shape=pltpu.HBM((var_count, own, peers * width), BF16),
        scratch_shapes=[pltpu.SemaphoreType.DMA((peers,))],
        input_output_aliases={1 + peers: 0} if more else {},
        compiler_params=params(),
    )(me, *in_vmem(blocks), *more)


def swapped(value, axis, distance):
    pairs = [(i, i ^ distance) for i in range(lax.axis_size(axis))]
    return lax.ppermute(value, axis, pairs)


def exchanged(blocks, axis):
    return lax.all_to_all(blocks, axis, split_axis=0, concat_axis=0, tiled=True)


def traded(blocks, order):
    out = list(blocks)
    for s in order:
        out[s] = swapped(blocks[s], "member", s)
    return out


def shards(ensemble, obs_weights, obs_tiles, obs_values, obs_error, obs_noise):
    peers = lax.axis_size("member")
    regions = lax.axis_size("region")
    var_count, _, tile_count = ensemble.shape
    width = tile_count // peers
    me = lax.axis_index("member").astype(jnp.int32)[None]
    region = lax.axis_index("region").astype(jnp.int32)
    tiles, values, error = (a[None, :] for a in (obs_tiles, obs_values, obs_error))
    *blocks, partial = pack(me, ensemble, obs_weights, tiles, peers)
    other = swapped(partial, "depth", 1)
    noises = traded([scale(obs_noise, error)] * peers, (1, 3, 2))
    predicted = traded([join(partial, other)] * peers, (1, 3, 2))
    pairs = [(i, i + 1) for i in range(1, regions - 1, 2)]
    pairs += [(j, i) for i, j in pairs]
    packet, sums = stats(me, predicted, values, error, tiles, regions)
    near = swapped(packet, "region", 1)
    far = lax.ppermute(packet, "region", pairs)
    states = traded([ensemble, *blocks], (1, 3, 2))
    all_sums = exchanged(sums, "region")
    noise = join_noise(noises)
    near_noise = swapped(noise, "region", 1)
    far_noise = lax.ppermute(noise, "region", pairs)
    side = 1 - 2 * (region % 2)
    offset = jnp.stack([me[0] * width, jnp.zeros_like(side), side, -side])
    anom_0 = prepare((packet, near))
    half = (var_count + 1) // 2
    anom_2, taper, means, anomalies, gain, packets, rest = start_gains(
        offset, states, (packet, near, far), anom_0, half, tile_count
    )
    ready, perturbed, root, inflation = first_updates(
        means, anomalies, gain, packets, far, all_sums, (noise, near_noise, far_noise), peers
    )
    shared = (anom_0, anom_2, taper)
    early = traded(ready, (1, 3, 2))
    ready = second_updates(rest, perturbed, root, shared)
    late = traded(ready, (1, 3, 2))
    output = place(me, early, 0, var_count)
    output = place(me, late, half, var_count, output)
    return (output, inflation.reshape(()))


def solution(mesh):
    return jax.shard_map(
        shards,
        mesh=mesh,
        in_specs=(
            P("depth", "member", "region"),
            P("depth"),
            P("region"),
            P("region"),
            P("region"),
            P("member", "region"),
        ),
        out_specs=(P("depth", "member", "region"), P()),
        check_vma=False,
    )
```
